128 devices in a mesh: pod: 1, dp: 64 (over z, y, x), tp: 2 (over core).
Axes of the slice: x: 4, y: 4, z: 4, core: 2. Of those that a mesh axis runs over, the one named last changes fastest.
Arguments:
- x_in: bfloat16 [128, 1024, 1024], P(('pod', 'dp'))
- seg_ids: int32 [128, 1024], P(('pod', 'dp'))
- gain_one: bfloat16 [1024], replicated
- gain_two: bfloat16 [1024], replicated
- w_qkv: bfloat16 [1024, 3072], P(None, 'tp')
- w_out: bfloat16 [16, 64, 1024], P('tp')
- w_up: bfloat16 [1024, 4096], P(None, 'tp')
- w_down: bfloat16 [4096, 1024], P('tp')
- grad_y: bfloat16 [128, 1024, 1024], P(('pod', 'dp'))
Outputs:
- output 1: bfloat16 [128, 1024, 1024], P(('pod', 'dp'))
- output 2: bfloat16 [128, 1024, 1024], P(('pod', 'dp'))
- output 3: bfloat16 [1024], P('pod')
- output 4: bfloat16 [1024], P('pod')
- output 5: bfloat16 [1024, 3072], P('pod', 'tp')
- output 6: bfloat16 [16, 64, 1024], P(('pod', 'tp'))
- output 7: bfloat16 [1024, 4096], P('pod', 'tp')
- output 8: bfloat16 [4096, 1024], P(('pod', 'tp'))
All inputs are finite; a program needn't handle non-finite values.
Results may differ from the reference program's by a relative error of at most 0.02.
Values are sent between devices in bfloat16 or wider.
A program may use at most 1 GiB of HBM per device.

```python
import functools
import jax
import jax.numpy as jnp
from jax import lax

BATCH_ROWS = 128
SEQ_LEN = 1024
HIDDEN_DIM = 1024
NUM_HEADS = 16
HEAD_DIM = 64
FFN_DIM = 4096
EPS_NORM = 1e-5


def setup_inputs(seed: int = 0, part: int = 0) -> dict:
    own_key = jax.random.fold_in(jax.random.key(seed), part)
    own_keys = jax.random.split(own_key, 3)
    shared_keys = jax.random.split(jax.random.key(seed + 1), 5)
    x_in = jax.random.normal(own_keys[0], (BATCH_ROWS, SEQ_LEN, HIDDEN_DIM), jnp.float32)
    cut_points = jax.random.randint(own_keys[1], (BATCH_ROWS, 3), 1, SEQ_LEN)
    positions = jnp.arange(SEQ_LEN)
    seg_ids = jnp.sum((positions[None, :, None] >= cut_points[:, None, :]).astype(jnp.int32), axis=-1)
    grad_y = jax.random.normal(own_keys[2], (BATCH_ROWS, SEQ_LEN, HIDDEN_DIM), jnp.float32)
    gain_pair = 1.0 + 0.3 * jax.random.normal(shared_keys[0], (2, HIDDEN_DIM), jnp.float32)
    qk_boost = jnp.array([1.5, 1.5, 1.0], jnp.float32)[None, None, :, None]
    w_qkv = jax.random.normal(shared_keys[1], (HIDDEN_DIM, NUM_HEADS, 3, HEAD_DIM), jnp.float32) * qk_boost * HIDDEN_DIM ** -0.5
    w_out = jax.random.normal(shared_keys[2], (NUM_HEADS, HEAD_DIM, HIDDEN_DIM), jnp.float32) * (2.0 * (NUM_HEADS * HEAD_DIM) ** -0.5)
    w_up = jax.random.normal(shared_keys[3], (HIDDEN_DIM, FFN_DIM), jnp.float32) * HIDDEN_DIM ** -0.5
    w_down = jax.random.normal(shared_keys[4], (FFN_DIM, HIDDEN_DIM), jnp.float32) * FFN_DIM ** -0.5
    return {
        "x_in": x_in.astype(jnp.bfloat16),
        "seg_ids": seg_ids,
        "gain_one": gain_pair[0].astype(jnp.bfloat16),
        "gain_two": gain_pair[1].astype(jnp.bfloat16),
        "w_qkv": w_qkv.reshape(HIDDEN_DIM, 3 * NUM_HEADS * HEAD_DIM).astype(jnp.bfloat16),
        "w_out": w_out.astype(jnp.bfloat16),
        "w_up": w_up.astype(jnp.bfloat16),
        "w_down": w_down.astype(jnp.bfloat16),
        "grad_y": grad_y.astype(jnp.bfloat16),
    }


def layer_norm(x_rows, gain_vec):
    x_f32 = x_rows.astype(jnp.float32)
    centered = x_f32 - jnp.mean(x_f32, axis=-1, keepdims=True)
    variance = jnp.mean(centered * centered, axis=-1, keepdims=True)
    return (centered * lax.rsqrt(variance + EPS_NORM) * gain_vec.astype(jnp.float32)).astype(jnp.bfloat16)


def head_attention(qkv_item, seg_row):
    scores = jnp.dot(qkv_item[0], qkv_item[1].T, preferred_element_type=jnp.float32) * (HEAD_DIM ** -0.5)
    positions = jnp.arange(SEQ_LEN)
    allowed = (positions[:, None] >= positions[None, :]) & (seg_row[:, None] == seg_row[None, :])
    attn_probs = jax.nn.softmax(jnp.where(allowed, scores, -1e30), axis=-1)
    return jnp.dot(attn_probs.astype(jnp.bfloat16), qkv_item[2], preferred_element_type=jnp.float32).astype(jnp.bfloat16)


def layer_forward(seg_ids, x_in, gain_one, gain_two, w_qkv, w_out, w_up, w_down):
    tokens = BATCH_ROWS * SEQ_LEN
    x_rows = x_in.reshape(tokens, HIDDEN_DIM)
    normed_a = layer_norm(x_rows, gain_one)
    qkv_rows = jnp.dot(normed_a, w_qkv, preferred_element_type=jnp.float32).astype(jnp.bfloat16)
    qkv_rows = qkv_rows.reshape(BATCH_ROWS, SEQ_LEN, NUM_HEADS, 3, HEAD_DIM)
    qkv_rows = jnp.transpose(qkv_rows, (0, 2, 3, 1, 4)).reshape(BATCH_ROWS * NUM_HEADS, 3, SEQ_LEN, HEAD_DIM)
    seg_rep = jnp.repeat(seg_ids, NUM_HEADS, axis=0)
    attn_out = lax.map(lambda map_item: jax.checkpoint(head_attention)(map_item[0], map_item[1]), (qkv_rows, seg_rep))
    attn_out = jnp.transpose(attn_out.reshape(BATCH_ROWS, NUM_HEADS, SEQ_LEN, HEAD_DIM), (0, 2, 1, 3)).reshape(tokens, NUM_HEADS * HEAD_DIM)
    part_one = jnp.dot(attn_out, w_out.reshape(NUM_HEADS * HEAD_DIM, HIDDEN_DIM), preferred_element_type=jnp.float32).astype(jnp.bfloat16)
    x_one = (x_rows.astype(jnp.float32) + part_one.astype(jnp.float32)).astype(jnp.bfloat16)
    normed_b = layer_norm(x_one, gain_two)
    pre_act = jnp.dot(normed_b, w_up, preferred_element_type=jnp.float32)
    hidden_act = jax.nn.gelu(pre_act, approximate=True).astype(jnp.bfloat16)
    part_two = jnp.dot(hidden_act, w_down, preferred_element_type=jnp.float32).astype(jnp.bfloat16)
    y_rows = (x_one.astype(jnp.float32) + part_two.astype(jnp.float32)).astype(jnp.bfloat16)
    return y_rows.reshape(BATCH_ROWS, SEQ_LEN, HIDDEN_DIM)


def reference(x_in, seg_ids, gain_one, gain_two, w_qkv, w_out, w_up, w_down, grad_y):
    y_out, pullback = jax.vjp(functools.partial(layer_forward, seg_ids), x_in, gain_one, gain_two, w_qkv, w_out, w_up, w_down)
    grad_list = pullback(grad_y)
    return (y_out, grad_list[0], grad_list[1], grad_list[2], grad_list[3], grad_list[4], grad_list[5], grad_list[6])
```

```python
import functools
import math

import jax
import jax.numpy as jnp
from jax import lax
from jax.experimental import pallas as pl
from jax.experimental.pallas import tpu as pltpu
from jax.sharding import PartitionSpec as P

EPS_NORM = 1e-5
NEG_LARGE = -1e30
LOG2E = math.log2(math.e)
SWAP = [(0, 1), (1, 0)]
TILE = 256
BF16 = jnp.bfloat16
F32 = jnp.float32


def norm_stats(x_rows):
    x_f32 = x_rows.astype(F32)
    mean = jnp.mean(x_f32, axis=-1, keepdims=True)
    centered = x_f32 - mean
    inv_std = lax.rsqrt(jnp.mean(centered * centered, axis=-1, keepdims=True) + EPS_NORM)
    return mean, inv_std


def norm_apply(x_rows, mean, inv_std, gain_vec):
    return ((x_rows.astype(F32) - mean) * inv_std * gain_vec.astype(F32)).astype(BF16)


def norm_backward(grad_out, x_rows, mean, inv_std, gain_vec):
    grad_f32 = grad_out.astype(F32)
    x_hat = (x_rows.astype(F32) - mean) * inv_std
    grad_gain = jnp.sum(grad_f32 * x_hat, axis=0)
    grad_hat = grad_f32 * gain_vec.astype(F32)
    mean_one = jnp.mean(grad_hat, axis=-1, keepdims=True)
    mean_two = jnp.mean(grad_hat * x_hat, axis=-1, keepdims=True)
    return inv_std * (grad_hat - mean_one - x_hat * mean_two), grad_gain


def dot_nn(lhs, rhs):
    return lax.dot_general(lhs, rhs, (((1,), (0,)), ((), ())), preferred_element_type=F32)


def dot_nt(lhs, rhs):
    return lax.dot_general(lhs, rhs, (((1,), (1,)), ((), ())), preferred_element_type=F32)


def dot_tn(lhs, rhs):
    return lax.dot_general(lhs, rhs, (((0,), (0,)), ((), ())), preferred_element_type=F32)


def attn_fwd_kernel(dim, scale, start_ref, qkv_ref, out_ref, lse_ref):
    seq = qkv_ref.shape[0]
    block = qkv_ref[...]
    block_t = block.T
    start = start_ref[0:1, :]
    heads_t = []
    for head in range(2):
        base = 3 * dim * head
        k_rows = block[:, base + dim : base + 2 * dim]
        q_cols = block_t[base : base + dim]
        v_cols = block_t[base + 2 * dim : base + 3 * dim]
        strips = []
        for i in range(seq // TILE):
            lo, hi = i * TILE, (i + 1) * TILE
            scores = dot_nn(k_rows[:hi], q_cols[:, lo:hi]) * (scale * LOG2E)
            k_pos = lax.broadcasted_iota(jnp.int32, (hi, TILE), 0)
            allowed = k_pos >= start[:, lo:hi]
            q_pos = lax.broadcasted_iota(jnp.int32, (TILE, TILE), 1) + lo
            diag = jnp.where(allowed[lo:] & (k_pos[lo:] <= q_pos), scores[lo:], NEG_LARGE)
            if lo:
                body = jnp.where(allowed[:lo], scores[:lo], NEG_LARGE)
                scores = jnp.concatenate([body, diag], axis=0)
            else:
                scores = diag
            top = jnp.max(scores, axis=0, keepdims=True)
            probs = jnp.exp2(scores - top)
            total = jnp.sum(probs, axis=0, keepdims=True)
            probs = (probs * (1.0 / total)).astype(BF16)
            strips.append(dot_nn(v_cols[:, :hi], probs))
            lse_ref[0, head : head + 1, lo:hi] = top + jnp.log2(total)
        heads_t.append(jnp.concatenate(strips, axis=1))
    out_ref[...] = jnp.concatenate(heads_t, axis=0).T.astype(BF16)


def attn_bwd_kernel(dim, scale, start_ref, qkv_ref, out_ref, grad_ref, lse_ref, dqkv_ref):
    seq = qkv_ref.shape[0]
    block = qkv_ref[...]
    block_t = block.T
    grad = grad_ref[...]
    grad_t = grad.T
    prod_t = grad_t.astype(F32) * out_ref[...].T.astype(F32)
    start = start_ref[0:1, :]
    pieces = []
    for head in range(2):
        base = 3 * dim * head
        q_rows = block[:, base : base + dim]
        k_rows = block[:, base + dim : base + 2 * dim]
        v_rows = block[:, base + 2 * dim : base + 3 * dim]
        q_cols = block_t[base : base + dim]
        k_cols = block_t[base + dim : base + 2 * dim]
        do_rows = grad[:, head * dim : (head + 1) * dim]
        do_cols = grad_t[head * dim : (head + 1) * dim]
        delta = jnp.sum(prod_t[head * dim : (head + 1) * dim], axis=0, keepdims=True)
        lse = lse_ref[0, head : head + 1, :]
        dq_cols = None
        dk_parts, dv_parts = [], []
        for j in range(seq // TILE):
            lo, hi = j * TILE, (j + 1) * TILE
            width = seq - lo
            scores = dot_nn(k_rows[lo:hi], q_cols[:, lo:]) * (scale * LOG2E)
            grad_probs = dot_nn(v_rows[lo:hi], do_cols[:, lo:])
            k_pos = lax.broadcasted_iota(jnp.int32, (TILE, width), 0) + lo
            allowed = k_pos >= start[:, lo:]
            q_pos = lax.broadcasted_iota(jnp.int32, (TILE, TILE), 1) + lo
            probs = jnp.exp2(scores - lse[:, lo:])
            diag = jnp.where(allowed[:, :TILE] & (k_pos[:, :TILE] <= q_pos), probs[:, :TILE], 0.0)
            if width > TILE:
                body = jnp.where(allowed[:, TILE:], probs[:, TILE:], 0.0)
                probs = jnp.concatenate([diag, body], axis=1)
            else:
                probs = diag
            grad_scores = (probs * (grad_probs - delta[:, lo:]) * scale).astype(BF16)
            dv_parts.append(dot_nn(probs.astype(BF16), do_rows[lo:]))
            dk_parts.append(dot_nn(grad_scores, q_rows[lo:]))
            dq_part = dot_nn(k_cols[:, lo:hi], grad_scores)
            if dq_cols is None:
                dq_cols = dq_part
            else:
                dq_cols = jnp.concatenate([dq_cols[:, :lo], dq_cols[:, lo:] + dq_part], axis=1)
        pieces.append(dq_cols.T)
        pieces.append(jnp.concatenate(dk_parts, axis=0))
        pieces.append(jnp.concatenate(dv_parts, axis=0))
    dqkv_ref[...] = jnp.concatenate(pieces, axis=1).astype(BF16)


def attn_specs(seq, dim, width):
    pairs = width // (6 * dim)
    start_spec = pl.BlockSpec((8, seq), lambda i: (0, 0))
    qkv_spec = pl.BlockSpec((seq, 6 * dim), lambda i: (0, i))
    out_spec = pl.BlockSpec((seq, 2 * dim), lambda i: (0, i))
    lse_spec = pl.BlockSpec((1, 8, seq), lambda i: (i, 0, 0))
    return pairs, start_spec, qkv_spec, out_spec, lse_spec


VMEM_LIMIT = 56 * 1024 * 1024


def attention_forward(start, qkv, dim, scale):
    seq, width = qkv.shape
    pairs, start_spec, qkv_spec, out_spec, lse_spec = attn_specs(seq, dim, width)
    return pl.pallas_call(
        functools.partial(attn_fwd_kernel, dim, scale),
        grid=(pairs,),
        in_specs=[start_spec, qkv_spec],
        out_specs=[out_spec, lse_spec],
        out_shape=[
            jax.ShapeDtypeStruct((seq, pairs * 2 * dim), BF16),
            jax.ShapeDtypeStruct((pairs, 8, seq), F32),
        ],
        compiler_params=pltpu.CompilerParams(vmem_limit_bytes=VMEM_LIMIT),
        cost_estimate=pl.CostEstimate(flops=pairs * 8 * seq * seq * dim, bytes_accessed=8 * seq * width // 3, transcendentals=pairs * seq * seq),
        name="attn_fwd",
    )(start, qkv)


def attention_backward(start, qkv, out, grad, lse, dim, scale):
    seq, width = qkv.shape
    pairs, start_spec, qkv_spec, out_spec, lse_spec = attn_specs(seq, dim, width)
    return pl.pallas_call(
        functools.partial(attn_bwd_kernel, dim, scale),
        grid=(pairs,),
        in_specs=[start_spec, qkv_spec, out_spec, out_spec, lse_spec],
        out_specs=qkv_spec,
        out_shape=jax.ShapeDtypeStruct((seq, width), BF16),
        compiler_params=pltpu.CompilerParams(vmem_limit_bytes=VMEM_LIMIT),
        cost_estimate=pl.CostEstimate(flops=pairs * 20 * seq * seq * dim, bytes_accessed=16 * seq * width // 3, transcendentals=pairs * seq * seq),
        name="attn_bwd",
    )(start, qkv, out, grad, lse)


GELU_A = math.sqrt(2.0 / math.pi)
GELU_B = 0.044715


def mlp_mid_kernel(rows, b_ref, dy_ref, up_ref, down_ref, act_ref, dpre_ref):
    for r in range(b_ref.shape[0] // rows):
        span = pl.ds(r * rows, rows)
        pre = dot_nn(b_ref[span, :], up_ref[...])
        grad_h = dot_nt(dy_ref[span, :], down_ref[...]).astype(BF16).astype(F32)
        square = pre * pre
        tanh = jnp.tanh(pre * (GELU_A + (GELU_A * GELU_B) * square))
        cdf = 0.5 + 0.5 * tanh
        act_ref[span, :] = (pre * cdf).astype(BF16)
        slope = cdf + (0.5 * pre) * (1.0 - tanh * tanh) * (GELU_A + (3.0 * GELU_A * GELU_B) * square)
        dpre_ref[span, :] = (grad_h * slope).astype(BF16)


def mlp_mid(normed, grad_rows, w_up, w_down, tile_n=512, rows=256):
    tokens, hidden = normed.shape
    ffn = w_up.shape[1]
    return pl.pallas_call(
        functools.partial(mlp_mid_kernel, rows),
        grid=(ffn // tile_n,),
        in_specs=[
            pl.BlockSpec((tokens, hidden), lambda i: (0, 0)),
            pl.BlockSpec((tokens, hidden), lambda i: (0, 0)),
            pl.BlockSpec((hidden, tile_n), lambda i: (0, i)),
            pl.BlockSpec((tile_n, hidden), lambda i: (i, 0)),
        ],
        out_specs=[pl.BlockSpec((tokens, tile_n), lambda i: (0, i))] * 2,
        out_shape=[jax.ShapeDtypeStruct((tokens, ffn), BF16)] * 2,
        compiler_params=pltpu.CompilerParams(vmem_limit_bytes=VMEM_LIMIT),
        cost_estimate=pl.CostEstimate(flops=4 * tokens * hidden * ffn, bytes_accessed=2 * tokens * (2 * hidden + 2 * ffn) + 4 * hidden * ffn, transcendentals=tokens * ffn),
        name="mlp_mid",
    )(normed, grad_rows, w_up, w_down)


MESH_ID = pl.DeviceIdType.MESH
RING = 4
FLOW_ROWS = 1024
FLOW_COLS = 1024
STREAMS = 2
STREAM_COLS = FLOW_COLS // STREAMS
LEVEL_ROWS = (256, 64, 16)
LEVEL_SLOT = (0, 768, 960)
SLOT_ROWS = 1008
AXIS_STRIDE = (1, 4, 16)
FLOWS = tuple((tuple((first + k) % 3 for k in range(3)), sign) for first in range(3) for sign in (1, -1))
STEPS = 6 * (RING - 1)


def hbm_block(refs, flow, stream, row, rows):
    down, up, qkv, out = refs
    lane = stream * STREAM_COLS
    if flow < 2:
        return down.at[pl.ds(flow * FLOW_ROWS + row, rows), pl.ds(lane, STREAM_COLS)]
    if flow < 4:
        return up.at[pl.ds(row, rows), pl.ds((flow - 2) * FLOW_COLS + lane, STREAM_COLS)]
    if flow == 4:
        return qkv.at[pl.ds(row, rows), pl.ds(lane, STREAM_COLS)]
    if stream == 0:
        return qkv.at[pl.ds(row, rows), pl.ds(FLOW_COLS, STREAM_COLS)]
    half = row // 512
    return out.at[pl.ds(pl.multiple_of(row - half * 512, 256), rows), pl.ds(pl.multiple_of(half * STREAM_COLS, STREAM_COLS), STREAM_COLS)]


def all_reduce_kernel(*refs):
    ins, outs = refs[:4], refs[4:8]
    own, slots, full, send_sem, recv_sem, load_sem, store_sem = refs[8:]
    me = lax.axis_index("dp")
    coords = (lax.rem(me, 4), lax.rem(me // 4, 4), me // 16)

    def neighbour(axis, sign):
        moved = lax.rem(coords[axis] + sign + RING, RING)
        return me + (moved - coords[axis]) * AXIS_STRIDE[axis]

    barrier = pltpu.get_barrier_semaphore()
    for axis in range(3):
        for sign in (1, -1):
            pl.semaphore_signal(barrier, inc=1, device_id={"dp": neighbour(axis, sign)}, device_id_type=MESH_ID)

    place, bases = [], []
    for axes, sign in FLOWS:
        spots = [coords[a] if sign > 0 else lax.rem(RING - coords[a], RING) for a in axes]
        base = [0]
        for level in range(2):
            base.append(base[-1] + lax.rem(spots[level] + 1, RING) * LEVEL_ROWS[level])
        place.append(spots)
        bases.append(base)

    def chunk(flow, level, shift):
        index = lax.rem(place[flow][level] + shift + RING, RING)
        return pl.multiple_of(bases[flow][level] + index * LEVEL_ROWS[level], LEVEL_ROWS[level])

    def view(ref, flow, stream, row, rows):
        return ref.at[flow, pl.ds(row, rows), pl.ds(stream * STREAM_COLS, STREAM_COLS)]

    def load(flow, stream, turn):
        row = chunk(flow, 0, -turn)
        return pltpu.make_async_copy(
            hbm_block(ins, flow, stream, row, LEVEL_ROWS[0]), view(own, flow, stream, row, LEVEL_ROWS[0]), load_sem.at[flow, stream, turn])

    def store(flow, stream, turn):
        row = chunk(flow, 0, 1 - turn)
        return pltpu.make_async_copy(
            view(full, flow, stream, row, LEVEL_ROWS[0]), hbm_block(outs, flow, stream, row, LEVEL_ROWS[0]), store_sem.at[flow, stream, turn])

    def where(step):
        if step < 9:
            return step // 3, step % 3, False
        return 2 - (step - 9) // 3, step % 3, True

    def copy(flow, stream, step):
        level, turn, gathering = where(step)
        rows = LEVEL_ROWS[level]
        axes, sign = FLOWS[flow]
        if gathering:
            source = view(full, flow, stream, chunk(flow, level, 1 - turn), rows)
            target = source
        else:
            source = view(own, flow, stream, chunk(flow, level, -turn), rows)
            target = view(slots, flow, stream, LEVEL_SLOT[level] + turn * rows, rows)
        return pltpu.make_async_remote_copy(
            src_ref=source, dst_ref=target, send_sem=send_sem.at[flow, stream, step], recv_sem=recv_sem.at[flow, stream, step],
            device_id={"dp": neighbour(axes[level], sign)}, device_id_type=MESH_ID)

    def absorb(flow, stream, step):
        level, turn, gathering = where(step)
        copy(flow, stream, step).wait_recv()
        lanes = pl.ds(stream * STREAM_COLS, STREAM_COLS)
        if gathering:
            if level == 1 and turn == 2:
                store(flow, stream, 0).start()
            if level == 0:
                store(flow, stream, turn + 1).start()
            return
        if level == 0:
            load(flow, stream, turn + 1).wait()
        rows = LEVEL_ROWS[level]
        row = chunk(flow, level, -turn - 1)
        last = step == 8
        part = min(rows, 64)

        def add(i, carry):
            at = pl.ds(pl.multiple_of(row + i * part, 16), part)
            got = slots[flow, pl.ds(pl.multiple_of(LEVEL_SLOT[level] + turn * rows + i * part, 16), part), lanes]
            total = (own[flow, at, lanes].astype(F32) + got.astype(F32)).astype(BF16)
            if last:
                full[flow, at, lanes] = total
            else:
                own[flow, at, lanes] = total
            return carry

        if rows == part:
            add(0, 0)
        else:
            lax.fori_loop(0, rows // part, add, 0)

    for turn in range(4):
        for stream in range(STREAMS):
            for flow in range(6):
                load(flow, stream, turn).start()
    pl.semaphore_wait(barrier, 6)
    for step in range(STEPS + 1):
        for stream in range(STREAMS):
            for flow in range(6):
                if step == 0:
                    load(flow, stream, 0).wait()
                else:
                    absorb(flow, stream, step - 1)
            if step < STEPS:
                for flow in range(6):
                    copy(flow, stream, step).start()
    for stream in range(STREAMS):
        for flow in range(6):
            for step in range(STEPS):
                copy(flow, stream, step).wait_send()
            for turn in range(4):
                store(flow, stream, turn).wait()


def all_reduce_dp(arrays):
    any_spec = pl.BlockSpec(memory_space=pl.ANY)
    flow_shape = (6, FLOW_ROWS, FLOW_COLS)
    return pl.pallas_call(
        all_reduce_kernel,
        in_specs=[any_spec] * 4,
        out_specs=[any_spec] * 4,
        out_shape=[jax.ShapeDtypeStruct(a.shape, a.dtype) for a in arrays],
        scratch_shapes=[
            pltpu.VMEM(flow_shape, BF16),
            pltpu.VMEM((6, SLOT_ROWS, FLOW_COLS), BF16),
            pltpu.VMEM(flow_shape, BF16),
            pltpu.SemaphoreType.DMA((6, STREAMS, STEPS)),
            pltpu.SemaphoreType.DMA((6, STREAMS, STEPS)),
            pltpu.SemaphoreType.DMA((6, STREAMS, 4)),
            pltpu.SemaphoreType.DMA((6, STREAMS, 4)),
        ],
        compiler_params=pltpu.CompilerParams(collective_id=0, has_side_effects=True, vmem_limit_bytes=VMEM_LIMIT),
        name="all_reduce_dp",
    )(*arrays)


def solution(mesh):
    batch_spec = P(("pod", "dp"), None, None)
    seg_spec = P(("pod", "dp"), None)

    def local_step(x_in, seg_ids, gain_one, gain_two, w_qkv, w_out, w_up, w_down, grad_y):
        heads_loc, dim, hidden = w_out.shape
        scale = dim ** -0.5
        swap = lambda value: lax.ppermute(value, "tp", SWAP)
        mine = lax.axis_index("tp")
        own_row = lambda value: lax.dynamic_index_in_dim(value, mine, 0, keepdims=False)

        w_out = w_out.reshape(heads_loc * dim, hidden)
        wqkv_p = swap(w_qkv)
        wout_p = swap(w_out)
        wup_p = swap(w_up)
        wdown_p = swap(w_down)
        x_rows = own_row(x_in)
        grad_rows = own_row(grad_y)
        seg = own_row(seg_ids)
        seq = x_rows.shape[0]
        start = jnp.sum((seg[None, :] < seg[:, None]).astype(jnp.int32), axis=1)
        start = jnp.broadcast_to(start[None, :], (8, seq))

        mean_a, inv_a = norm_stats(x_rows)
        normed_a = norm_apply(x_rows, mean_a, inv_a, gain_one)
        qkv_o = dot_nn(normed_a, w_qkv).astype(BF16)
        attn_o, lse_o = attention_forward(start, qkv_o, dim, scale)
        qkv_p = dot_nn(normed_a, wqkv_p).astype(BF16)
        attn_p, lse_p = attention_forward(start, qkv_p, dim, scale)
        part_one = (dot_nn(attn_o, w_out) + dot_nn(attn_p, wout_p)).astype(BF16)
        x_one = (x_rows.astype(F32) + part_one.astype(F32)).astype(BF16)
        mean_b, inv_b = norm_stats(x_one)
        normed_b = norm_apply(x_one, mean_b, inv_b, gain_two)

        act_p, dpre_p = mlp_mid(normed_b, grad_rows, wup_p, wdown_p)
        act_o, dpre_o = mlp_mid(normed_b, grad_rows, w_up, w_down)
        sent_down = swap(dot_tn(act_p, grad_rows).astype(BF16))
        sent_up = swap(dot_tn(normed_b, dpre_p).astype(BF16))
        grad_down = (dot_tn(act_o, grad_rows) + sent_down.astype(F32)).astype(BF16)
        grad_up = (dot_tn(normed_b, dpre_o) + sent_up.astype(F32)).astype(BF16)

        grad_norm_b = (dot_nt(dpre_o, w_up) + dot_nt(dpre_p, wup_p)).astype(BF16)
        back_b, gain_grad_two = norm_backward(grad_norm_b, x_one, mean_b, inv_b, gain_two)
        grad_x_one = (grad_rows.astype(F32) + back_b).astype(BF16)
        dattn_o = dot_nt(grad_x_one, w_out).astype(BF16)
        dattn_p = dot_nt(grad_x_one, wout_p).astype(BF16)
        sent_out = swap(dot_tn(attn_p, grad_x_one).astype(BF16))
        grad_out_w = (dot_tn(attn_o, grad_x_one) + sent_out.astype(F32)).astype(BF16)
        dqkv_p = attention_backward(start, qkv_p, attn_p, dattn_p, lse_p, dim, scale)
        dqkv_o = attention_backward(start, qkv_o, attn_o, dattn_o, lse_o, dim, scale)
        sent_qkv = swap(dot_tn(normed_a, dqkv_p).astype(BF16))
        grad_wqkv = (dot_tn(normed_a, dqkv_o) + sent_qkv.astype(F32)).astype(BF16)

        part_two = (dot_nn(act_o, w_down) + dot_nn(act_p, wdown_p)).astype(BF16)
        y_rows = (x_one.astype(F32) + part_two.astype(F32)).astype(BF16)
        grad_norm_a = (dot_nt(dqkv_o, w_qkv) + dot_nt(dqkv_p, wqkv_p)).astype(BF16)
        back_a, gain_grad_one = norm_backward(grad_norm_a, x_rows, mean_a, inv_a, gain_one)
        grad_x = (grad_x_one.astype(F32) + back_a).astype(BF16)

        def both_rows(value):
            other = swap(value)
            first = mine == 0
            return jnp.stack([jnp.where(first, value, other), jnp.where(first, other, value)])

        sum_down, sum_up, sum_qkv, sum_out = all_reduce_dp((grad_down, grad_up, grad_wqkv, grad_out_w))
        weight_grads = (sum_qkv, sum_out, sum_up, sum_down)
        gain_grads = lax.psum((gain_grad_one, gain_grad_two), ("dp", "tp"))
        return (
            both_rows(y_rows),
            both_rows(grad_x),
            gain_grads[0].astype(BF16),
            gain_grads[1].astype(BF16),
            weight_grads[0],
            weight_grads[1].reshape(heads_loc, dim, hidden),
            weight_grads[2],
            weight_grads[3],
        )

    return jax.shard_map(
        local_step,
        mesh=mesh,
        in_specs=(batch_spec, seg_spec, P(None), P(None), P(None, "tp"), P("tp", None, None), P(None, "tp"), P("tp", None), batch_spec),
        out_specs=(batch_spec, batch_spec, P("pod"), P("pod"), P("pod", "tp"), P(("pod", "tp"), None, None), P("pod", "tp"), P(("pod", "tp"), None)),
        check_vma=False,
    )
```

```python
import functools
import math

import jax
import jax.numpy as jnp
from jax import lax
from jax.experimental import pallas as pl
from jax.experimental.pallas import tpu as pltpu
from jax.sharding import PartitionSpec as P

EPS_NORM = 1e-5
NEG_LARGE = -1e30
LOG2E = math.log2(math.e)
SWAP = [(0, 1), (1, 0)]
TILE = 256
BF16 = jnp.bfloat16
F32 = jnp.float32


def norm_stats(x_rows):
    x_f32 = x_rows.astype(F32)
    mean = jnp.mean(x_f32, axis=-1, keepdims=True)
    centered = x_f32 - mean
    inv_std = lax.rsqrt(jnp.mean(centered * centered, axis=-1, keepdims=True) + EPS_NORM)
    return mean, inv_std


def norm_apply(x_rows, mean, inv_std, gain_vec):
    return ((x_rows.astype(F32) - mean) * inv_std * gain_vec.astype(F32)).astype(BF16)


def norm_backward(grad_out, x_rows, mean, inv_std, gain_vec):
    grad_f32 = grad_out.astype(F32)
    x_hat = (x_rows.astype(F32) - mean) * inv_std
    grad_gain = jnp.sum(grad_f32 * x_hat, axis=0)
    grad_hat = grad_f32 * gain_vec.astype(F32)
    mean_one = jnp.mean(grad_hat, axis=-1, keepdims=True)
    mean_two = jnp.mean(grad_hat * x_hat, axis=-1, keepdims=True)
    return inv_std * (grad_hat - mean_one - x_hat * mean_two), grad_gain


def dot_nn(lhs, rhs):
    return lax.dot_general(lhs, rhs, (((1,), (0,)), ((), ())), preferred_element_type=F32)


def dot_nt(lhs, rhs):
    return lax.dot_general(lhs, rhs, (((1,), (1,)), ((), ())), preferred_element_type=F32)


def dot_tn(lhs, rhs):
    return lax.dot_general(lhs, rhs, (((0,), (0,)), ((), ())), preferred_element_type=F32)


VMEM_LIMIT = 56 * 1024 * 1024
TAIL_VMEM = 63 * 1024 * 1024


def attn_fwd_kernel(dim, scale, start_ref, normed_ref, wp_ref, wo_ref, qkv_ref, out_ref, lse_ref, normed_t_ref):
    seq = qkv_ref.shape[0]
    step = pl.program_id(0)
    half = pl.num_programs(0) // 2

    @pl.when(step == 0)
    def _():
        normed_t_ref[...] = normed_ref[...].T

    weight = jnp.where(step < half, wp_ref[...], wo_ref[...])
    block = dot_nn(normed_ref[...], weight).astype(BF16)
    qkv_ref[...] = block
    block_t = block.T
    start = start_ref[0:1, :]
    heads_t = []
    for head in range(2):
        base = 3 * dim * head
        k_rows = block[:, base + dim : base + 2 * dim]
        q_cols = block_t[base : base + dim]
        v_cols = block_t[base + 2 * dim : base + 3 * dim]
        strips = []
        for i in range(seq // TILE):
            lo, hi = i * TILE, (i + 1) * TILE
            scores = dot_nn(k_rows[:hi], q_cols[:, lo:hi]) * (scale * LOG2E)
            k_pos = lax.broadcasted_iota(jnp.int32, (hi, TILE), 0)
            allowed = k_pos >= start[:, lo:hi]
            q_pos = lax.broadcasted_iota(jnp.int32, (TILE, TILE), 1) + lo
            diag = jnp.where(allowed[lo:] & (k_pos[lo:] <= q_pos), scores[lo:], NEG_LARGE)
            if lo:
                body = jnp.where(allowed[:lo], scores[:lo], NEG_LARGE)
                scores = jnp.concatenate([body, diag], axis=0)
            else:
                scores = diag
            top = jnp.max(scores, axis=0, keepdims=True)
            probs = jnp.exp2(scores - top)
            total = jnp.sum(probs, axis=0, keepdims=True)
            probs = (probs * (1.0 / total)).astype(BF16)
            strips.append(dot_nn(v_cols[:, :hi], probs))
            lse_ref[0, head : head + 1, lo:hi] = top + jnp.log2(total)
        heads_t.append(jnp.concatenate(strips, axis=1))
    out_ref[...] = jnp.concatenate(heads_t, axis=0).T.astype(BF16)


def attention_forward(start, normed, w_peer, w_own, dim, scale):
    seq, hidden = normed.shape
    width = 6 * dim
    half = w_own.shape[1] // width
    pairs = 2 * half
    return pl.pallas_call(
        functools.partial(attn_fwd_kernel, dim, scale),
        grid=(pairs,),
        in_specs=[
            pl.BlockSpec((8, seq), lambda i: (0, 0)),
            pl.BlockSpec((seq, hidden), lambda i: (0, 0)),
            pl.BlockSpec((hidden, width), lambda i: (0, jnp.minimum(i, half - 1))),
            pl.BlockSpec((hidden, width), lambda i: (0, jnp.maximum(i - half, 0))),
        ],
        out_specs=[
            pl.BlockSpec((seq, width), lambda i: (0, i)),
            pl.BlockSpec((seq, 2 * dim), lambda i: (0, i)),
            pl.BlockSpec((1, 8, seq), lambda i: (i, 0, 0)),
            pl.BlockSpec((hidden, seq), lambda i: (0, 0)),
        ],
        out_shape=[
            jax.ShapeDtypeStruct((seq, pairs * width), BF16),
            jax.ShapeDtypeStruct((seq, pairs * 2 * dim), BF16),
            jax.ShapeDtypeStruct((pairs, 8, seq), F32),
            jax.ShapeDtypeStruct((hidden, seq), BF16),
        ],
        compiler_params=pltpu.CompilerParams(vmem_limit_bytes=VMEM_LIMIT),
        cost_estimate=pl.CostEstimate(flops=pairs * (8 * seq * seq * dim + 2 * seq * hidden * width), bytes_accessed=4 * seq * pairs * width, transcendentals=pairs * seq * seq),
        name="attn_fwd",
    )(start, normed, w_peer, w_own)


def attn_bwd_head(dim, scale, head, block, block_t, grad, grad_t, prod_t, start, lse):
    seq = block.shape[0]
    base = 3 * dim * head
    q_rows = block[:, base : base + dim]
    k_rows = block[:, base + dim : base + 2 * dim]
    v_rows = block[:, base + 2 * dim : base + 3 * dim]
    q_cols = block_t[base : base + dim]
    k_cols = block_t[base + dim : base + 2 * dim]
    do_rows = grad[:, head * dim : (head + 1) * dim]
    do_cols = grad_t[head * dim : (head + 1) * dim]
    delta = jnp.sum(prod_t[head * dim : (head + 1) * dim], axis=0, keepdims=True)
    dq_cols = None
    dk_parts, dv_parts = [], []
    for j in range(seq // TILE):
        lo, hi = j * TILE, (j + 1) * TILE
        width = seq - lo
        scores = dot_nn(k_rows[lo:hi], q_cols[:, lo:]) * (scale * LOG2E)
        grad_probs = dot_nn(v_rows[lo:hi], do_cols[:, lo:])
        k_pos = lax.broadcasted_iota(jnp.int32, (TILE, width), 0) + lo
        allowed = k_pos >= start[:, lo:]
        q_pos = lax.broadcasted_iota(jnp.int32, (TILE, TILE), 1) + lo
        probs = jnp.exp2(scores - lse[:, lo:])
        diag = jnp.where(allowed[:, :TILE] & (k_pos[:, :TILE] <= q_pos), probs[:, :TILE], 0.0)
        if width > TILE:
            body = jnp.where(allowed[:, TILE:], probs[:, TILE:], 0.0)
            probs = jnp.concatenate([diag, body], axis=1)
        else:
            probs = diag
        grad_scores = (probs * (grad_probs - delta[:, lo:]) * scale).astype(BF16)
        dv_parts.append(dot_nn(probs.astype(BF16), do_rows[lo:]))
        dk_parts.append(dot_nn(grad_scores, q_rows[lo:]))
        dq_part = dot_nn(k_cols[:, lo:hi], grad_scores)
        if dq_cols is None:
            dq_cols = dq_part
        else:
            dq_cols = jnp.concatenate([dq_cols[:, :lo], dq_cols[:, lo:] + dq_part], axis=1)
    return [dq_cols.T, jnp.concatenate(dk_parts, axis=0), jnp.concatenate(dv_parts, axis=0)]


GELU_A = math.sqrt(2.0 / math.pi)
GELU_B = 0.044715


def mlp_mid_kernel(rows, b_ref, dy_ref, up_ref, down_ref, act_ref, dpre_ref):
    for r in range(b_ref.shape[0] // rows):
        span = pl.ds(r * rows, rows)
        pre = dot_nn(b_ref[span, :], up_ref[...])
        grad_h = dot_nt(dy_ref[span, :], down_ref[...]).astype(BF16).astype(F32)
        square = pre * pre
        tanh = jnp.tanh(pre * (GELU_A + (GELU_A * GELU_B) * square))
        cdf = 0.5 + 0.5 * tanh
        act_ref[span, :] = (pre * cdf).astype(BF16)
        slope = cdf + (0.5 * pre) * (1.0 - tanh * tanh) * (GELU_A + (3.0 * GELU_A * GELU_B) * square)
        dpre_ref[span, :] = (grad_h * slope).astype(BF16)


def mlp_mid(normed, grad_rows, w_up, w_down, tile_n=512, rows=256):
    tokens, hidden = normed.shape
    ffn = w_up.shape[1]
    return pl.pallas_call(
        functools.partial(mlp_mid_kernel, rows),
        grid=(ffn // tile_n,),
        in_specs=[
            pl.BlockSpec((tokens, hidden), lambda i: (0, 0)),
            pl.BlockSpec((tokens, hidden), lambda i: (0, 0)),
            pl.BlockSpec((hidden, tile_n), lambda i: (0, i)),
            pl.BlockSpec((tile_n, hidden), lambda i: (i, 0)),
        ],
        out_specs=[pl.BlockSpec((tokens, tile_n), lambda i: (0, i))] * 2,
        out_shape=[jax.ShapeDtypeStruct((tokens, ffn), BF16)] * 2,
        compiler_params=pltpu.CompilerParams(vmem_limit_bytes=VMEM_LIMIT),
        cost_estimate=pl.CostEstimate(flops=4 * tokens * hidden * ffn, bytes_accessed=2 * tokens * (2 * hidden + 2 * ffn) + 4 * hidden * ffn, transcendentals=tokens * ffn),
        name="mlp_mid",
    )(normed, grad_rows, w_up, w_down)


MESH_ID = pl.DeviceIdType.MESH
RING = 4
FLOW_ROWS = 1024
UNIT = 128
BIG_UNITS = 6
SMALL_UNITS = 2
STREAMS = 2
LEVEL_ROWS = (256, 64, 16)
LEVEL_SLOT = (0, 768, 960)
SLOT_ROWS = 1008
AXIS_STRIDE = (1, 4, 16)
FLOWS = tuple((tuple((first + k) % 3 for k in range(3)), sign) for first in range(3) for sign in (1, -1))
STEPS = 6 * (RING - 1)
POINTS = 4
FREED = {4: 0, 7: 1, 9: 2}
PAIR_US = 7.5
HOP_US = 3.0
GRADS_UP, GRADS_DOWN, GRADS_OUT = range(3)


def big_pieces(flow):
    first = flow * BIG_UNITS
    bounds = ((GRADS_UP, 0, 16), (GRADS_DOWN, 16, 24), (GRADS_DOWN, 24, 32), (GRADS_OUT, 32, 36))
    pieces = []
    for array, begin, end in bounds:
        lo, hi = max(first, begin), min(first + BIG_UNITS, end)
        if lo < hi:
            origin = 16 if array == GRADS_DOWN else begin
            pieces.append((array, lo - origin, (lo - first) * UNIT, (hi - lo) * UNIT))
    return pieces


def hbm_block(refs, piece, row, rows):
    array, local, _, width = piece
    ref = refs[array]
    if array == GRADS_UP:
        return ref.at[pl.ds(row, rows), pl.ds(local * UNIT, width)]
    if array == GRADS_DOWN:
        return ref.at[pl.ds((local // 8) * FLOW_ROWS + row, rows), pl.ds((local % 8) * UNIT, width)]
    half = row // 512
    lane = pl.multiple_of(half * 512 + local * UNIT, UNIT)
    return ref.at[pl.ds(pl.multiple_of(row - half * 512, 256), rows), pl.ds(lane, width)]


def plan_ops(pairs):
    inside, after = {}, []
    for stream in range(STREAMS):
        unit = (0.0330, 0.0110)[stream]
        clock = (0.0, pairs * PAIR_US)[stream]
        for step in range(STEPS + 1):
            point = None
            for pair in range(pairs):
                for spot in range(POINTS):
                    at = (pair + (0.0, 0.33, 0.67, 0.84)[spot]) * PAIR_US
                    if point is None and at >= clock - 0.01:
                        point, when = (pair, spot), at
            if point is None:
                when = max(clock, pairs * PAIR_US)
                after.append((when, stream, step))
            else:
                inside.setdefault(point, []).append((stream, step))
            level = min(step // 3 if step < 9 else 2 - (step - 9) // 3, 2)
            clock = when + HOP_US + unit * LEVEL_ROWS[max(level, 0)]
    after.sort()
    return inside, [(stream, step) for _, stream, step in after]


def tail_kernel(dim, scale, pairs, *refs):
    (start_ref, qkv_ref, out_ref, grad_ref, lse_ref, wp_ref, wo_ref, normed_t_ref, x_ref, gx_ref, gain_ref, gain_two_ref) = refs[:12]
    ins, outs = refs[12:15], refs[15:18]
    qkv_sum, dx_out, gains_out = refs[18:21]
    (own, slots, small, small_slots, sent, da_acc, dx_buf, gains, send_sem, recv_sem, load_sem, store_sem, swap_send, swap_recv, dx_sem, gain_send, gain_recv, free_sem) = refs[21:]
    pid = pl.program_id(0)
    half = pairs // 2
    me = lax.axis_index("dp")
    core = lax.axis_index("tp")
    coords = (lax.rem(me, 4), lax.rem(me // 4, 4), me // 16)
    inside, after = plan_ops(pairs)

    def neighbour(axis, shift):
        moved = lax.rem(coords[axis] + shift + RING, RING)
        return {"dp": me + (moved - coords[axis]) * AXIS_STRIDE[axis]}

    partner = {"tp": 1 - core}
    place, bases = [], []
    for axes, sign in FLOWS:
        spots = [coords[a] if sign > 0 else lax.rem(RING - coords[a], RING) for a in axes]
        base = [0]
        for level in range(2):
            base.append(base[-1] + lax.rem(spots[level] + 1, RING) * LEVEL_ROWS[level])
        place.append(spots)
        bases.append(base)

    def chunk(flow, level, shift):
        index = lax.rem(place[flow][level] + shift + RING, RING)
        return pl.multiple_of(bases[flow][level] + index * LEVEL_ROWS[level], LEVEL_ROWS[level])

    def view(of_slots, flow, stream, row, rows):
        if stream == 0:
            return (slots if of_slots else own).at[flow, pl.ds(row, rows), :]
        return (small_slots if of_slots else small).at[pl.ds(SMALL_UNITS * flow, SMALL_UNITS), pl.ds(row, rows), :]

    def loads(flow, turn):
        row = chunk(flow, 0, -turn)
        copies = []
        for k, piece in enumerate(big_pieces(flow)):
            target = own.at[flow, pl.ds(row, LEVEL_ROWS[0]), pl.ds(piece[2], piece[3])]
            copies.append(pltpu.make_async_copy(hbm_block(ins, piece, row, LEVEL_ROWS[0]), target, load_sem.at[flow, turn, k]))
        return copies

    def stores(flow, stream, turn):
        row = chunk(flow, 0, 1 - turn)
        copies = []
        if stream == 1:
            for k in range(SMALL_UNITS):
                index = SMALL_UNITS * flow + k
                target = qkv_sum.at[pl.ds(row, LEVEL_ROWS[0]), pl.ds(index * UNIT, UNIT)]
                copies.append(pltpu.make_async_copy(small.at[index, pl.ds(row, LEVEL_ROWS[0]), :], target, store_sem.at[flow, stream, turn, k]))
            return copies
        for k, piece in enumerate(big_pieces(flow)):
            source = own.at[flow, pl.ds(row, LEVEL_ROWS[0]), pl.ds(piece[2], piece[3])]
            copies.append(pltpu.make_async_copy(source, hbm_block(outs, piece, row, LEVEL_ROWS[0]), store_sem.at[flow, stream, turn, k]))
        return copies

    def where(step):
        if step < 9:
            return step // 3, step % 3, False
        return 2 - (step - 9) // 3, step % 3, True

    def copy(flow, stream, step):
        level, turn, gathering = where(step)
        rows = LEVEL_ROWS[level]
        axes, sign = FLOWS[flow]
        if gathering:
            source = view(False, flow, stream, chunk(flow, level, 1 - turn), rows)
            target = source
        else:
            source = view(False, flow, stream, chunk(flow, level, -turn), rows)
            target = view(True, flow, stream, LEVEL_SLOT[level] + turn * rows, rows)
        return pltpu.make_async_remote_copy(
            src_ref=source, dst_ref=target, send_sem=send_sem.at[flow, stream, step], recv_sem=recv_sem.at[flow, stream, step],
            device_id=neighbour(axes[level], sign), device_id_type=MESH_ID)

    def absorb(flow, stream, step):
        level, turn, gathering = where(step)
        copy(flow, stream, step).wait_recv()
        if gathering:
            if level == 1 and turn == 2:
                for each in stores(flow, stream, 0):
                    each.start()
            if level == 0:
                for each in stores(flow, stream, turn + 1):
                    each.start()
            return
        if level == 0 and stream == 0:
            for each in loads(flow, turn + 1):
                each.wait()
        rows = LEVEL_ROWS[level]
        row = chunk(flow, level, -turn - 1)
        part = min(rows, 64)

        def add(i, carry):
            kept = view(False, flow, stream, pl.multiple_of(row + i * part, 16), part)
            got = view(True, flow, stream, pl.multiple_of(LEVEL_SLOT[level] + turn * rows + i * part, 16), part)
            kept[...] = (kept[...].astype(F32) + got[...].astype(F32)).astype(BF16)
            return carry

        if rows == part:
            add(0, 0)
        else:
            lax.fori_loop(0, rows // part, add, 0)

    def run_op(stream, step):
        for flow in range(6):
            if step > 0:
                absorb(flow, stream, step - 1)
            elif stream == 0:
                for each in loads(flow, 0):
                    each.wait()
        if step in FREED:
            level = FREED[step]
            for flow, (axes, sign) in enumerate(FLOWS):
                for turn in range(3):
                    copy(flow, stream, 3 * level + turn).wait_send()
                pl.semaphore_signal(free_sem.at[flow, stream, level], inc=1, device_id=neighbour(axes[level], -sign), device_id_type=MESH_ID)
        if step in (9, 12, 15):
            for flow in range(6):
                pl.semaphore_wait(free_sem.at[flow, stream, 2 - (step - 9) // 3], 1)
        if step < STEPS:
            for flow in range(6):
                copy(flow, stream, step).start()

    def run_point(spot):
        for pair in range(pairs):
            ops = inside.get((pair, spot), [])
            if ops:
                @pl.when(pid == pair)
                def _():
                    for stream, step in ops:
                        run_op(stream, step)

    def swap_copy(j):
        return pltpu.make_async_remote_copy(
            src_ref=sent.at[lax.rem(j, 2)], dst_ref=small.at[pl.ds(3 * j, 3)], send_sem=swap_send.at[j], recv_sem=swap_recv.at[j],
            device_id=partner, device_id_type=MESH_ID)

    @pl.when(pid == 0)
    def _():
        barrier = pltpu.get_barrier_semaphore()
        for axis in range(3):
            for shift in (1, 2, 3):
                pl.semaphore_signal(barrier, inc=1, device_id=neighbour(axis, shift), device_id_type=MESH_ID)
        pl.semaphore_signal(barrier, inc=1, device_id=partner, device_id_type=MESH_ID)
        for turn in range(4):
            for flow in range(6):
                for each in loads(flow, turn):
                    each.start()
        pl.semaphore_wait(barrier, 10)
        da_acc[...] = jnp.zeros_like(da_acc)

    run_point(0)
    block = qkv_ref[...]
    block_t = block.T
    grad = grad_ref[...]
    grad_t = grad.T
    prod_t = grad_t.astype(F32) * out_ref[...].T.astype(F32)
    start = start_ref[0:1, :]
    pieces = attn_bwd_head(dim, scale, 0, block, block_t, grad, grad_t, prod_t, start, lse_ref[0, 0:1, :])
    run_point(1)
    pieces += attn_bwd_head(dim, scale, 1, block, block_t, grad, grad_t, prod_t, start, lse_ref[0, 1:2, :])
    dqkv = jnp.concatenate(pieces, axis=1).astype(BF16)
    run_point(2)
    weight = jnp.where(pid < half, wp_ref[...], wo_ref[...])
    da_acc[...] += dot_nt(dqkv, weight)
    run_point(3)

    @pl.when(pid < half)
    def _():
        @pl.when(pid >= 2)
        def _():
            swap_copy(pid - 2).wait_send()

        dw = dot_nn(normed_t_ref[...], dqkv).astype(BF16)
        for k in range(3):
            sent[lax.rem(pid, 2), k] = dw[:, k * UNIT : (k + 1) * UNIT]
        swap_copy(pid).start()

    @pl.when(pid >= half)
    def _():
        j = pid - half

        @pl.when(j < 2)
        def _():
            swap_copy(j + half - 2).wait_send()

        swap_copy(j).wait_recv()
        dw = dot_nn(normed_t_ref[...], dqkv)
        for k in range(3):
            index = 3 * j + k
            small[index] = (dw[:, k * UNIT : (k + 1) * UNIT] + small[index].astype(F32)).astype(BF16)

    @pl.when(pid == pairs - 1)
    def _():
        queue = list(after)

        def advance(count):
            for _ in range(min(count, len(queue))):
                run_op(*queue.pop(0))

        advance(1)
        gain = gain_ref[0:1, :]
        tile = 128

        def norm_tile(i, total):
            at = pl.ds(pl.multiple_of(i * tile, tile), tile)
            x_f32 = x_ref[at, :].astype(F32)
            centered = x_f32 - jnp.mean(x_f32, axis=-1, keepdims=True)
            inv_std = lax.rsqrt(jnp.mean(centered * centered, axis=-1, keepdims=True) + EPS_NORM)
            x_hat = centered * inv_std
            grad_a = da_acc[at, :].astype(BF16).astype(F32)
            grad_hat = grad_a * gain
            mean_one = jnp.mean(grad_hat, axis=-1, keepdims=True)
            mean_two = jnp.mean(grad_hat * x_hat, axis=-1, keepdims=True)
            back = inv_std * (grad_hat - mean_one - x_hat * mean_two)
            dx_buf[at, :] = (gx_ref[at, :].astype(F32) + back).astype(BF16)
            return total + jnp.sum(grad_a * x_hat, axis=0, keepdims=True)

        gain_one = lax.fori_loop(0, x_ref.shape[0] // tile, norm_tile, jnp.zeros_like(gain))
        for k in range(8):
            gains[0, core, k : k + 1, :] = gain_one[:, k * UNIT : (k + 1) * UNIT]
            gains[0, core, k + 8 : k + 9, :] = gain_two_ref[0:1, k * UNIT : (k + 1) * UNIT]
        advance(1)
        dx_local = pltpu.make_async_copy(dx_buf, dx_out.at[core], dx_sem.at[0])
        dx_remote = pltpu.make_async_remote_copy(
            src_ref=dx_buf, dst_ref=dx_out.at[core], send_sem=dx_sem.at[1], recv_sem=dx_sem.at[2], device_id=partner, device_id_type=MESH_ID)
        dx_local.start()
        dx_remote.start()

        def gain_copy(stage, slot, where_to, lane):
            return pltpu.make_async_remote_copy(
                src_ref=gains.at[stage, slot], dst_ref=gains.at[stage, slot], send_sem=gain_send.at[stage, lane], recv_sem=gain_recv.at[stage, slot],
                device_id=where_to, device_id_type=MESH_ID)

        for stage in range(4):
            if stage == 0:
                members, spot = 2, core
                others = [(partner, 1 - core)]
            else:
                members, spot = RING, coords[stage - 1]
                others = [(neighbour(stage - 1, d), lax.rem(spot + d, RING)) for d in (1, 2, 3)]
            for lane, (target, _) in enumerate(others):
                gain_copy(stage, spot, target, lane).start()
            advance(3)
            for lane, (target, slot) in enumerate(others):
                gain_copy(stage, slot, target, lane).wait_recv()
                gain_copy(stage, spot, target, lane).wait_send()
            total = gains[stage, 0]
            for member in range(1, members):
                total = total + gains[stage, member]
            if stage < 3:
                gains[stage + 1, coords[stage]] = total
            else:
                gains_out[...] = total
        advance(len(queue))
        dx_local.wait()
        dx_remote.wait()
        for stream in range(STREAMS):
            for flow in range(6):
                for step in range(9, STEPS):
                    copy(flow, stream, step).wait_send()
                for turn in range(4):
                    for each in stores(flow, stream, turn):
                        each.wait()


def backward_tail(dim, scale, start, qkv, out, grad, lse, w_peer, w_own, normed_t, x_rows, gx_rows, gain_one, gain_two_grad, grads):
    seq, hidden = x_rows.shape
    width = 6 * dim
    half = w_own.shape[1] // width
    pairs = 2 * half
    any_spec = pl.BlockSpec(memory_space=pl.ANY)
    fixed = lambda shape: pl.BlockSpec(shape, lambda i: (0,) * len(shape), pipeline_mode=pl.Buffered(1))
    row = lambda value: jnp.broadcast_to(value.astype(F32)[None, :], (8, hidden))
    return pl.pallas_call(
        functools.partial(tail_kernel, dim, scale, pairs),
        grid=(pairs,),
        in_specs=[
            fixed((8, seq)),
            pl.BlockSpec((seq, width), lambda i: (0, i)),
            pl.BlockSpec((seq, 2 * dim), lambda i: (0, i)),
            pl.BlockSpec((seq, 2 * dim), lambda i: (0, i)),
            pl.BlockSpec((1, 8, seq), lambda i: (i, 0, 0)),
            pl.BlockSpec((hidden, width), lambda i: (0, jnp.minimum(i, half - 1))),
            pl.BlockSpec((hidden, width), lambda i: (0, jnp.maximum(i - half, 0))),
            fixed((hidden, seq)),
            fixed((seq, hidden)),
            fixed((seq, hidden)),
            fixed((8, hidden)),
            fixed((8, hidden)),
        ] + [any_spec] * 3,
        out_specs=[any_spec] * 5 + [pl.BlockSpec((16, UNIT), lambda i: (0, 0))],
        out_shape=[jax.ShapeDtypeStruct(g.shape, BF16) for g in grads] + [
            jax.ShapeDtypeStruct((hidden, half * width), BF16),
            jax.ShapeDtypeStruct((2, seq, hidden), BF16),
            jax.ShapeDtypeStruct((16, UNIT), F32),
        ],
        scratch_shapes=[
            pltpu.VMEM((6, FLOW_ROWS, BIG_UNITS * UNIT), BF16),
            pltpu.VMEM((6, SLOT_ROWS, BIG_UNITS * UNIT), BF16),
            pltpu.VMEM((12, FLOW_ROWS, UNIT), BF16),
            pltpu.VMEM((12, SLOT_ROWS, UNIT), BF16),
            pltpu.VMEM((2, 3, FLOW_ROWS, UNIT), BF16),
            pltpu.VMEM((seq, hidden), F32),
            pltpu.VMEM((seq, hidden), BF16),
            pltpu.VMEM((4, RING, 16, UNIT), F32),
            pltpu.SemaphoreType.DMA((6, STREAMS, STEPS)),
            pltpu.SemaphoreType.DMA((6, STREAMS, STEPS)),
            pltpu.SemaphoreType.DMA((6, 4, 3)),
            pltpu.SemaphoreType.DMA((6, STREAMS, 4, 3)),
            pltpu.SemaphoreType.DMA((half,)),
            pltpu.SemaphoreType.DMA((half,)),
            pltpu.SemaphoreType.DMA((3,)),
            pltpu.SemaphoreType.DMA((4, 3)),
            pltpu.SemaphoreType.DMA((4, RING)),
            pltpu.SemaphoreType.REGULAR((6, STREAMS, 3)),
        ],
        compiler_params=pltpu.CompilerParams(collective_id=0, has_side_effects=True, vmem_limit_bytes=TAIL_VMEM),
        cost_estimate=pl.CostEstimate(flops=pairs * (20 * seq * seq * dim + 4 * seq * hidden * width), bytes_accessed=32 * seq * width, transcendentals=pairs * seq * seq),
        name="backward_tail",
    )(start, qkv, out, grad, lse, w_peer, w_own, normed_t, x_rows, gx_rows, row(gain_one), row(gain_two_grad), *grads)


def solution(mesh):
    batch_spec = P(("pod", "dp"), None, None)
    seg_spec = P(("pod", "dp"), None)

    def local_step(x_in, seg_ids, gain_one, gain_two, w_qkv, w_out, w_up, w_down, grad_y):
        heads_loc, dim, hidden = w_out.shape
        scale = dim ** -0.5
        swap = lambda value: lax.ppermute(value, "tp", SWAP)
        mine = lax.axis_index("tp")
        own_row = lambda value: lax.dynamic_index_in_dim(value, mine, 0, keepdims=False)

        w_out = w_out.reshape(heads_loc * dim, hidden)
        wqkv_p = swap(w_qkv)
        wout_p = swap(w_out)
        wup_p = swap(w_up)
        wdown_p = swap(w_down)
        x_rows = own_row(x_in)
        grad_rows = own_row(grad_y)
        seg = own_row(seg_ids)
        seq = x_rows.shape[0]
        start = jnp.sum((seg[None, :] < seg[:, None]).astype(jnp.int32), axis=1)
        start = jnp.broadcast_to(start[None, :], (8, seq))

        mean_a, inv_a = norm_stats(x_rows)
        normed_a = norm_apply(x_rows, mean_a, inv_a, gain_one)
        qkv, attn, lse, normed_t = attention_forward(start, normed_a, wqkv_p, w_qkv, dim, scale)
        wout_all = jnp.concatenate([wout_p, w_out], axis=0)
        part_one = dot_nn(attn, wout_all).astype(BF16)
        x_one = (x_rows.astype(F32) + part_one.astype(F32)).astype(BF16)
        mean_b, inv_b = norm_stats(x_one)
        normed_b = norm_apply(x_one, mean_b, inv_b, gain_two)

        act_p, dpre_p = mlp_mid(normed_b, grad_rows, wup_p, wdown_p)
        act_o, dpre_o = mlp_mid(normed_b, grad_rows, w_up, w_down)
        sent_down = swap(dot_tn(act_p, grad_rows).astype(BF16))
        sent_up = swap(dot_tn(normed_b, dpre_p).astype(BF16))
        grad_down = (dot_tn(act_o, grad_rows) + sent_down.astype(F32)).astype(BF16)
        grad_up = (dot_tn(normed_b, dpre_o) + sent_up.astype(F32)).astype(BF16)

        grad_norm_b = (dot_nt(dpre_o, w_up) + dot_nt(dpre_p, wup_p)).astype(BF16)
        back_b, gain_grad_two = norm_backward(grad_norm_b, x_one, mean_b, inv_b, gain_two)
        grad_x_one = (grad_rows.astype(F32) + back_b).astype(BF16)
        grad_wout = dot_tn(attn, grad_x_one)
        rows_loc = heads_loc * dim
        sent_out = swap(grad_wout[:rows_loc].astype(BF16))
        grad_out_w = (grad_wout[rows_loc:] + sent_out.astype(F32)).astype(BF16)
        dattn = dot_nt(grad_x_one, wout_all).astype(BF16)

        part_two = (dot_nn(act_o, w_down) + dot_nn(act_p, wdown_p)).astype(BF16)
        y_rows = (x_one.astype(F32) + part_two.astype(F32)).astype(BF16)

        def both_rows(value):
            other = swap(value)
            first = mine == 0
            return jnp.stack([jnp.where(first, value, other), jnp.where(first, other, value)])

        sum_up, sum_down, sum_out, sum_qkv, grad_x, gain_sums = backward_tail(
            dim, scale, start, qkv, attn, dattn, lse, wqkv_p, w_qkv, normed_t, x_rows, grad_x_one, gain_one, gain_grad_two, (grad_up, grad_down, grad_out_w))
        gain_sums = gain_sums.reshape(2, hidden).astype(BF16)
        return (
            both_rows(y_rows),
            grad_x,
            gain_sums[0],
            gain_sums[1],
            sum_qkv,
            sum_out.reshape(heads_loc, dim, hidden),
            sum_up,
            sum_down,
        )

    return jax.shard_map(
        local_step,
        mesh=mesh,
        in_specs=(batch_spec, seg_spec, P(None), P(None), P(None, "tp"), P("tp", None, None), P(None, "tp"), P("tp", None), batch_spec),
        out_specs=(batch_spec, batch_spec, P("pod"), P("pod"), P("pod", "tp"), P(("pod", "tp"), None, None), P("pod", "tp"), P(("pod", "tp"), None)),
        check_vma=False,
    )
```

```python
import functools
import math

import jax
import jax.numpy as jnp
from jax import lax
from jax.experimental import pallas as pl
from jax.experimental.pallas import tpu as pltpu
from jax.sharding import PartitionSpec as P

EPS_NORM = 1e-5
NEG_LARGE = -1e30
LOG2E = math.log2(math.e)
SWAP = [(0, 1), (1, 0)]
TILE = 256
FWD_TILE = 512
UNIT = 128
BF16 = jnp.bfloat16
F32 = jnp.float32
ALL = ...
ROW = dict(axis=-1, keepdims=True)
COL = dict(axis=0, keepdims=True)


def norm_stats(x_rows):
    x_f32 = x_rows.astype(F32)
    mean = jnp.mean(x_f32, **ROW)
    centered = x_f32 - mean
    inv_std = lax.rsqrt(jnp.mean(centered * centered, **ROW) + EPS_NORM)
    return mean, inv_std


def norm_apply(x_rows, mean, inv_std, gain_vec):
    return ((x_rows.astype(F32) - mean) * inv_std * gain_vec.astype(F32)).astype(BF16)


def norm_backward(grad_out, x_rows, mean, inv_std, gain_vec):
    grad_f32 = grad_out.astype(F32)
    x_hat = (x_rows.astype(F32) - mean) * inv_std
    grad_gain = jnp.sum(grad_f32 * x_hat, **COL)
    grad_hat = grad_f32 * gain_vec.astype(F32)
    mean_one = jnp.mean(grad_hat, **ROW)
    mean_two = jnp.mean(grad_hat * x_hat, **ROW)
    return inv_std * (grad_hat - mean_one - x_hat * mean_two), grad_gain


def cost(flops):
    return pl.CostEstimate(flops=flops, bytes_accessed=flops // UNIT, transcendentals=flops // UNIT)


def dot_nn(lhs, rhs):
    return lax.dot_general(lhs, rhs, (((1,), (0,)), ((), ())), preferred_element_type=F32)


def dot_nt(lhs, rhs):
    return lax.dot_general(lhs, rhs, (((1,), (1,)), ((), ())), preferred_element_type=F32)


def dot_tn(lhs, rhs):
    return lax.dot_general(lhs, rhs, (((0,), (0,)), ((), ())), preferred_element_type=F32)


FIRST = lambda i: (0, 0)
ACROSS = lambda i: (0, i)
VMEM_LIMIT = 56 * 1024 * 1024
TAIL_VMEM = 63 * 1024 * 1024


def head_parts(dim, head, width, take):
    base = head * (width // 2)
    return [take(lo, lo + dim) for lo in range(base, base + width // 2, dim)]


def attn_fwd_kernel(dim, scale, start_ref, normed_ref, wp_ref, wo_ref, qkv_ref, out_ref, lse_ref, normed_t_ref):
    seq = qkv_ref.shape[0]
    step = pl.program_id(0)
    half = pl.num_programs(0) // 2

    @pl.when(step == 0)
    def _():
        normed_t_ref[ALL] = normed_ref[ALL].T

    weight = jnp.where(step < half, wp_ref[ALL], wo_ref[ALL])
    block = dot_nn(normed_ref[ALL], weight).astype(BF16)
    qkv_ref[ALL] = block
    block_t = block.T
    start = start_ref[0:1, :]
    heads_t = []
    for head in range(2):
        _, k_rows, _ = head_parts(dim, head, block.shape[1], lambda lo, hi: block[:, lo:hi])
        q_cols, _, v_cols = head_parts(dim, head, block.shape[1], lambda lo, hi: block_t[lo:hi])
        strips = []
        for i in range(seq // FWD_TILE):
            lo, hi = i * FWD_TILE, (i + 1) * FWD_TILE
            scores = dot_nn(k_rows[:hi], q_cols[:, lo:hi]) * (scale * LOG2E)
            k_pos = lax.broadcasted_iota(jnp.int32, (hi, FWD_TILE), 0)
            allowed = k_pos >= start[:, lo:hi]
            q_pos = lax.broadcasted_iota(jnp.int32, (FWD_TILE, FWD_TILE), 1) + lo
            diag = jnp.where(allowed[lo:] & (k_pos[lo:] <= q_pos), scores[lo:], NEG_LARGE)
            if lo:
                body = jnp.where(allowed[:lo], scores[:lo], NEG_LARGE)
                scores = jnp.concatenate([body, diag], axis=0)
            else:
                scores = diag
            top = jnp.max(scores, **COL)
            probs = jnp.exp2(scores - top)
            total = jnp.sum(probs, **COL)
            probs = (probs * (1.0 / total)).astype(BF16)
            strips.append(dot_nn(v_cols[:, :hi], probs))
            lse_ref[0, head : head + 1, lo:hi] = top + jnp.log2(total)
        heads_t.append(jnp.concatenate(strips, axis=1))
    out_ref[ALL] = jnp.concatenate(heads_t, axis=0).T.astype(BF16)


def attention_forward(start, normed, w_peer, w_own, dim, scale):
    seq, hidden = normed.shape
    width = 6 * dim
    half = w_own.shape[1] // width
    pairs = 2 * half
    return pl.pallas_call(
        functools.partial(attn_fwd_kernel, dim, scale),
        grid=(pairs,),
        in_specs=[
            pl.BlockSpec((8, seq), FIRST),
            pl.BlockSpec((seq, hidden), FIRST),
            *half_specs((hidden, width), half, 1),
        ],
        out_specs=[
            pl.BlockSpec((seq, width), ACROSS),
            pl.BlockSpec((seq, 2 * dim), ACROSS),
            pl.BlockSpec((1, 8, seq), lambda i: (i, 0, 0)),
            pl.BlockSpec((hidden, seq), FIRST),
        ],
        out_shape=[
            jax.ShapeDtypeStruct((seq, pairs * width), BF16),
            jax.ShapeDtypeStruct((seq, pairs * 2 * dim), BF16),
            jax.ShapeDtypeStruct((pairs, 8, seq), F32),
            jax.ShapeDtypeStruct((hidden, seq), BF16),
        ],
        compiler_params=pltpu.CompilerParams(vmem_limit_bytes=VMEM_LIMIT),
        cost_estimate=cost(pairs * seq * seq * hidden),
        name="attn_fwd",
    )(start, normed, w_peer, w_own)


def attn_bwd_head(dim, scale, head, block, block_t, grad, grad_t, prod_t, start, lse):
    seq = block.shape[0]
    q_rows, k_rows, v_rows = head_parts(dim, head, block.shape[1], lambda lo, hi: block[:, lo:hi])
    q_cols, k_cols, _ = head_parts(dim, head, block.shape[1], lambda lo, hi: block_t[lo:hi])
    do_rows = grad[:, head * dim : (head + 1) * dim]
    do_cols = grad_t[head * dim : (head + 1) * dim]
    delta = jnp.sum(prod_t[head * dim : (head + 1) * dim], **COL)
    dq_cols = None
    dk_parts, dv_parts = [], []
    for j in range(seq // TILE):
        lo, hi = j * TILE, (j + 1) * TILE
        width = seq - lo
        scores = dot_nn(k_rows[lo:hi], q_cols[:, lo:]) * (scale * LOG2E)
        grad_probs = dot_nn(v_rows[lo:hi], do_cols[:, lo:])
        k_pos = lax.broadcasted_iota(jnp.int32, (TILE, width), 0) + lo
        allowed = k_pos >= start[:, lo:]
        q_pos = lax.broadcasted_iota(jnp.int32, (TILE, TILE), 1) + lo
        probs = jnp.exp2(scores - lse[:, lo:])
        diag = jnp.where(allowed[:, :TILE] & (k_pos[:, :TILE] <= q_pos), probs[:, :TILE], 0.0)
        if width > TILE:
            body = jnp.where(allowed[:, TILE:], probs[:, TILE:], 0.0)
            probs = jnp.concatenate([diag, body], axis=1)
        else:
            probs = diag
        grad_scores = (probs * (grad_probs - delta[:, lo:]) * scale).astype(BF16)
        dv_parts.append(dot_nn(probs.astype(BF16), do_rows[lo:]))
        dk_parts.append(dot_nn(grad_scores, q_rows[lo:]))
        dq_part = dot_nn(k_cols[:, lo:hi], grad_scores)
        if dq_cols is None:
            dq_cols = dq_part
        else:
            dq_cols = jnp.concatenate([dq_cols[:, :lo], dq_cols[:, lo:] + dq_part], axis=1)
    return [dq_cols.T, jnp.concatenate(dk_parts, axis=0), jnp.concatenate(dv_parts, axis=0)]


GELU_A = math.sqrt(2.0 / math.pi)
GELU_B = 0.044715


def mlp_mid_kernel(rows, b_ref, dy_ref, up_p_ref, up_o_ref, down_p_ref, down_o_ref, act_ref, dpre_ref):
    peer = pl.program_id(0) < pl.num_programs(0) // 2
    w_up = jnp.where(peer, up_p_ref[ALL], up_o_ref[ALL])
    w_down = jnp.where(peer, down_p_ref[ALL], down_o_ref[ALL])
    for r in range(b_ref.shape[0] // rows):
        span = pl.ds(r * rows, rows)
        pre = dot_nn(b_ref[span, :], w_up)
        grad_h = dot_nt(dy_ref[span, :], w_down).astype(BF16).astype(F32)
        square = pre * pre
        tanh = jnp.tanh(pre * (GELU_A + (GELU_A * GELU_B) * square))
        cdf = 0.5 + 0.5 * tanh
        act_ref[span, :] = (pre * cdf).astype(BF16)
        slope = cdf + (0.5 * pre) * (1.0 - tanh * tanh) * (GELU_A + (3.0 * GELU_A * GELU_B) * square)
        dpre_ref[span, :] = (grad_h * slope).astype(BF16)


def whole(shape):
    return pl.BlockSpec(shape, lambda i: (0,) * len(shape), pipeline_mode=pl.Buffered(1))


def half_specs(shape, half, axis):
    at = lambda index: (0, index) if axis else (index, 0)
    return [
        pl.BlockSpec(shape, lambda i: at(jnp.minimum(i, half - 1))),
        pl.BlockSpec(shape, lambda i: at(jnp.maximum(i - half, 0))),
    ]


def mlp_mid(normed, grad_rows, up_p, up_o, down_p, down_o, tile_n=512, rows=1024):
    tokens, hidden = normed.shape
    half = up_o.shape[1] // tile_n
    ffn = 2 * up_o.shape[1]
    return pl.pallas_call(
        functools.partial(mlp_mid_kernel, rows),
        grid=(2 * half,),
        in_specs=[pl.BlockSpec((tokens, hidden), FIRST)] * 2 + half_specs((hidden, tile_n), half, 1) + half_specs((tile_n, hidden), half, 0),
        out_specs=[pl.BlockSpec((tokens, tile_n), ACROSS)] * 2,
        out_shape=[jax.ShapeDtypeStruct((tokens, ffn), BF16)] * 2,
        compiler_params=pltpu.CompilerParams(vmem_limit_bytes=VMEM_LIMIT),
        cost_estimate=cost(tokens * hidden * ffn),
        name="mlp_mid",
    )(normed, grad_rows, up_p, up_o, down_p, down_o)


MESH_ID = pl.DeviceIdType.MESH
RING = 4
FLOW_ROWS = 1024
BIG_COLS = 6 * UNIT
BIG_BOUNDS = (0, 6, 12, 17, 22, 27, 32)
SMALL_BOUNDS = (None, (0, 2, 4, 6, 8, 9, 10), range(10, 17))
OUT_FIRST = 6
STREAMS = 3
LEVEL_ROWS = (256, 64, 16)
LEVEL_SLOT = (0, 768, 960)
SLOT_ROWS = 1008
BIG_SLOT_BASE = 768
AXIS_STRIDE = (1, 4, 16)
FLOWS = tuple((tuple((first + k) % 3 for k in range(3)), sign) for first in range(3) for sign in (1, -1))
FLOW_IDS = range(len(FLOWS))
PEERS = (1, 2, 3)
N_FLOWS = len(FLOWS)
TOP_ROWS, PART_ROWS = 256, 64
HALF_COLS = 512
STEPS = 10
SEMS = 18
POINTS = 4
FIRST_STEP = (3, 0, 0)
PAIR_US = 9.5
HOP_US = 3.2
STREAM_US = (1.4 * 6, 1.4 * 2, 1.4)
GRADS_UP, GRADS_DOWN = range(2)


def big_width(flow):
    return (BIG_BOUNDS[flow + 1] - BIG_BOUNDS[flow]) * UNIT


def big_pieces(flow):
    first, last = BIG_BOUNDS[flow], BIG_BOUNDS[flow + 1]
    pieces = []
    for array, begin, end in ((GRADS_UP, 0, 16), (GRADS_DOWN, 16, 24), (GRADS_DOWN, 24, 32)):
        lo, hi = max(first, begin), min(last, end)
        if lo < hi:
            pieces.append((array, lo - 16 if array == GRADS_DOWN else lo, (lo - first) * UNIT, (hi - lo) * UNIT))
    return pieces


def hbm_block(refs, piece, row, rows):
    array, local, _, width = piece
    ref = refs[array]
    if array == GRADS_UP:
        return ref.at[pl.ds(row, rows), pl.ds(local * UNIT, width)]
    return ref.at[pl.ds((local // 8) * FLOW_ROWS + row, rows), pl.ds((local % 8) * UNIT, width)]


def tell(semaphore, device):
    pl.semaphore_signal(semaphore, inc=1, device_id=device, device_id_type=MESH_ID)


def ring_tools():
    me = lax.axis_index("dp")
    coords = (lax.rem(me, 4), lax.rem(me // 4, 4), me // 16)

    def neighbour(axis, shift):
        moved = lax.rem(coords[axis] + shift + RING, RING)
        return {"dp": me + (moved - coords[axis]) * AXIS_STRIDE[axis]}

    place, bases = [], []
    for axes, sign in FLOWS:
        spots = [coords[a] if sign > 0 else lax.rem(RING - coords[a], RING) for a in axes]
        base = [0]
        for level in range(2):
            base.append(base[-1] + lax.rem(spots[level] + 1, RING) * LEVEL_ROWS[level])
        place.append(spots)
        bases.append(base)

    def chunk(flow, level, shift):
        index = lax.rem(place[flow][level] + shift + RING, RING)
        return pl.multiple_of(bases[flow][level] + index * LEVEL_ROWS[level], LEVEL_ROWS[level])

    return coords, neighbour, chunk


def mlp_out_kernel(steps, act_ref, dpre_ref, down_p_ref, down_o_ref, up_p_ref, up_o_ref, x_ref, up_hbm, down_hbm, db_ref, part_ref, y_out, own, slots, y_acc, b_acc, y_buf, send_sem, recv_sem, load_sem, y_sem):
    pid = pl.program_id(0)
    core = lax.axis_index("tp")
    partner = {"tp": 1 - core}
    coords, neighbour, chunk = ring_tools()
    ins = (up_hbm, down_hbm)
    rows = TOP_ROWS

    def lanes(flow, stream):
        middle = 3 * UNIT
        return pl.ds(0, middle) if stream == 0 else pl.ds(middle, big_width(flow) - middle)

    def loads(flow, turn):
        row = chunk(flow, 0, -turn)
        return [
            pltpu.make_async_copy(hbm_block(ins, piece, row, rows), own.at[flow, pl.ds(row, rows), pl.ds(piece[2], piece[3])], load_sem.at[flow, turn, k])
            for k, piece in enumerate(big_pieces(flow))
        ]

    def copy(flow, stream, turn):
        axes, sign = FLOWS[flow]
        return pltpu.make_async_remote_copy(
            src_ref=own.at[flow, pl.ds(chunk(flow, 0, -turn), rows), lanes(flow, stream)],
            dst_ref=slots.at[flow, pl.ds(turn * rows, rows), lanes(flow, stream)],
            send_sem=send_sem.at[flow, stream, turn], recv_sem=recv_sem.at[flow, stream, turn],
            device_id=neighbour(axes[0], sign), device_id_type=MESH_ID)

    def run_op(stream, step):
        for flow in FLOW_IDS:
            if step == 0:
                if stream == 0:
                    for each in loads(flow, 0):
                        each.wait()
                continue
            copy(flow, stream, step - 1).wait_recv()
            if stream == 0:
                for each in loads(flow, step):
                    each.wait()
            row = chunk(flow, 0, -step)

            def add(i, carry):
                at = (flow, pl.ds(pl.multiple_of(row + i * PART_ROWS, PART_ROWS), PART_ROWS), lanes(flow, stream))
                total = own[at].astype(F32) + slots[flow, pl.ds(pl.multiple_of((step - 1) * rows + i * PART_ROWS, PART_ROWS), PART_ROWS), lanes(flow, stream)].astype(F32)
                if step == 3:
                    part_ref[flow, pl.ds(pl.multiple_of(i * PART_ROWS, PART_ROWS), PART_ROWS), lanes(flow, stream)] = total.astype(BF16)
                else:
                    own[at] = total.astype(BF16)
                return carry

            lax.fori_loop(0, rows // PART_ROWS, add, 0)
        if step < 3:
            for flow in FLOW_IDS:
                copy(flow, stream, step).start()

    @pl.when(pid == 0)
    def _():
        barrier = pltpu.get_barrier_semaphore()
        for axis in range(3):
            for shift in (1, 3):
                tell(barrier, neighbour(axis, shift))
        tell(barrier, partner)
        for turn in range(4):
            for flow in FLOW_IDS:
                for each in loads(flow, turn):
                    each.start()
        pl.semaphore_wait(barrier, 7)
        y_acc[ALL] = jnp.zeros_like(y_acc)
        b_acc[ALL] = jnp.zeros_like(b_acc)
        run_op(0, 0)
        run_op(1, 0)

    @pl.when(pid == steps // 2)
    def _():
        run_op(0, 1)

    @pl.when(pid == steps - steps // 4)
    def _():
        run_op(1, 1)

    peer = pid < steps // 2
    y_acc[ALL] += dot_nn(act_ref[ALL], jnp.where(peer, down_p_ref[ALL], down_o_ref[ALL]))
    b_acc[ALL] += dot_nt(dpre_ref[ALL], jnp.where(peer, up_p_ref[ALL], up_o_ref[ALL]))

    @pl.when(pid == steps - 1)
    def _():
        run_op(0, 2)

        def tile(i, carry):
            at = pl.ds(pl.multiple_of(i * UNIT, UNIT), UNIT)
            y_buf[at, :] = (x_ref[at, :].astype(F32) + y_acc[at, :].astype(BF16).astype(F32)).astype(BF16)
            db_ref[at, :] = b_acc[at, :].astype(BF16)
            return carry

        lax.fori_loop(0, x_ref.shape[0] // UNIT, tile, 0)
        y_local = pltpu.make_async_copy(y_buf, y_out.at[core], y_sem.at[0])
        y_remote = pltpu.make_async_remote_copy(
            src_ref=y_buf, dst_ref=y_out.at[core], send_sem=y_sem.at[1], recv_sem=y_sem.at[2], device_id=partner, device_id_type=MESH_ID)
        y_local.start()
        y_remote.start()
        run_op(1, 2)
        run_op(0, 3)
        run_op(1, 3)
        y_local.wait()
        y_remote.wait()
        for flow in FLOW_IDS:
            for stream in range(2):
                for turn in range(3):
                    copy(flow, stream, turn).wait_send()


def mlp_out(act, dpre, down_p, down_o, up_p, up_o, x_one, grads, tile_n=1024):
    tokens, ffn = act.shape
    hidden = x_one.shape[1]
    steps = ffn // tile_n
    any_spec = pl.BlockSpec(memory_space=pl.ANY)
    return pl.pallas_call(
        functools.partial(mlp_out_kernel, steps),
        grid=(steps,),
        in_specs=[pl.BlockSpec((tokens, tile_n), ACROSS)] * 2
        + half_specs((tile_n, hidden), steps // 2, 0) + half_specs((hidden, tile_n), steps // 2, 1) + [whole((tokens, hidden)), any_spec, any_spec],
        out_specs=[whole((tokens, hidden)), whole((N_FLOWS, TOP_ROWS, BIG_COLS)), any_spec],
        out_shape=[
            jax.ShapeDtypeStruct((tokens, hidden), BF16),
            jax.ShapeDtypeStruct((N_FLOWS, TOP_ROWS, BIG_COLS), BF16),
            jax.ShapeDtypeStruct((2, tokens, hidden), BF16),
        ],
        scratch_shapes=[
            pltpu.VMEM((N_FLOWS, FLOW_ROWS, BIG_COLS), BF16),
            pltpu.VMEM((N_FLOWS, 3 * TOP_ROWS, BIG_COLS), BF16),
            pltpu.VMEM((tokens, hidden), F32),
            pltpu.VMEM((tokens, hidden), F32),
            pltpu.VMEM((tokens, hidden), BF16),
            pltpu.SemaphoreType.DMA((N_FLOWS, 2, 3)),
            pltpu.SemaphoreType.DMA((N_FLOWS, 2, 3)),
            pltpu.SemaphoreType.DMA((N_FLOWS, 4, 2)),
            pltpu.SemaphoreType.DMA((3,)),
        ],
        compiler_params=pltpu.CompilerParams(collective_id=1, has_side_effects=True, vmem_limit_bytes=TAIL_VMEM),
        cost_estimate=cost(tokens * hidden * ffn),
        name="mlp_out",
    )(act, dpre, down_p, down_o, up_p, up_o, x_one, *grads)


def plan_ops(pairs):
    inside, after = {}, []
    for stream in range(STREAMS):
        clock = (0.0, pairs // 2 * PAIR_US, pairs * PAIR_US)[stream]
        for step in range(FIRST_STEP[stream], STEPS + 1):
            point = None
            for pair in range(pairs):
                for spot in range(POINTS):
                    at = (pair + (0.0, 0.3, 0.55, 0.8)[spot]) * PAIR_US
                    if point is None and at >= clock - 0.01:
                        point, when = (pair, spot), at
            if point is None:
                when = max(clock, pairs * PAIR_US)
                after.append((when, stream, step))
            else:
                inside.setdefault(point, []).append((stream, step))
            if step < STEPS:
                clock = when + HOP_US + STREAM_US[stream]
    after.sort()
    return inside, [(stream, step) for _, stream, step in after]


def tail_kernel(dim, scale, pairs, *refs):
    (start_ref, qkv_ref, out_ref, grad_ref, lse_ref, wp_ref, wo_ref, normed_t_ref, x_ref, gx_ref, gain_ref, gain_two_ref) = refs[:12]
    (part_ref, out_hbm), outs = refs[12:14], refs[14:16]
    out_sum, qkv_sum, dx_out, gains_out = refs[16:20]
    (own, slots, small, small_slots, sent, da_acc, dx_buf, gains, send_sem, recv_sem, load_sem, store_sem, swap_send, swap_recv, dx_sem, gain_send, gain_recv, free_sem) = refs[20:]
    pid = pl.program_id(0)
    half = pairs // 2
    core = lax.axis_index("tp")
    coords, neighbour, chunk = ring_tools()
    inside, after = plan_ops(pairs)
    partner = {"tp": 1 - core}

    def view(of_slots, flow, stream, row, rows):
        if stream == 0:
            if of_slots:
                return slots.at[flow, pl.ds(row - BIG_SLOT_BASE, rows), pl.ds(0, big_width(flow))]
            return own.at[flow, pl.ds(row, rows), pl.ds(0, big_width(flow))]
        first, last = SMALL_BOUNDS[stream][flow : flow + 2]
        units = pl.ds(first, last - first)
        return (small_slots if of_slots else small).at[units, pl.ds(row, rows), :]

    def loads():
        copies = []
        for flow in FLOW_IDS:
            target = own.at[flow, pl.ds(chunk(flow, 0, 1), TOP_ROWS), :]
            copies.append(pltpu.make_async_copy(part_ref.at[flow], target, load_sem.at[flow]))
        for k in range(4):
            for side in range(2):
                source = out_hbm.at[:, pl.ds((4 * side + k) * UNIT, UNIT)]
                target = small.at[OUT_FIRST + k, pl.ds(side * 512, 512), :]
                copies.append(pltpu.make_async_copy(source, target, load_sem.at[6 + 2 * k + side]))
        return copies

    def stores(flow, stream, turn):
        row = chunk(flow, 0, 1 - turn)
        rows = TOP_ROWS
        copies = []
        if stream > 0:
            for k, index in enumerate(range(*SMALL_BOUNDS[stream][flow : flow + 2])):
                if OUT_FIRST <= index < OUT_FIRST + 4:
                    side = row // 512
                    lane = pl.multiple_of(side * 512 + (index - OUT_FIRST) * UNIT, UNIT)
                    target = out_sum.at[pl.ds(pl.multiple_of(row - side * 512, rows), rows), pl.ds(lane, UNIT)]
                else:
                    unit = index if index < OUT_FIRST else index - 4
                    target = qkv_sum.at[pl.ds(row, rows), pl.ds(unit * UNIT, UNIT)]
                copies.append(pltpu.make_async_copy(small.at[index, pl.ds(row, rows), :], target, store_sem.at[flow, stream, turn, k]))
            return copies
        for k, piece in enumerate(big_pieces(flow)):
            source = own.at[flow, pl.ds(row, rows), pl.ds(piece[2], piece[3])]
            copies.append(pltpu.make_async_copy(source, hbm_block(outs, piece, row, rows), store_sem.at[flow, stream, turn, k]))
        return copies

    def remote(flow, stream, source, target, index, axis, shift):
        return pltpu.make_async_remote_copy(
            src_ref=source, dst_ref=target, send_sem=send_sem.at[flow, stream, index], recv_sem=recv_sem.at[flow, stream, index],
            device_id=neighbour(axis, shift), device_id_type=MESH_ID)

    def direct_level(step):
        return step - 2 if step < 5 else 7 - step

    def copies(flow, stream, step):
        axes, sign = FLOWS[flow]
        if step < 3:
            rows = TOP_ROWS
            source = view(False, flow, stream, chunk(flow, 0, -step), rows)
            return [remote(flow, stream, source, view(True, flow, stream, step * rows, rows), step, axes[0], sign)]
        if step >= 7:
            source = view(False, flow, stream, chunk(flow, 0, 8 - step), TOP_ROWS)
            return [remote(flow, stream, source, source, step + 8, axes[0], sign)]
        level = direct_level(step)
        rows = LEVEL_ROWS[level]
        sends = []
        for d in PEERS:
            source = view(False, flow, stream, chunk(flow, level, d + 1 if step < 5 else 1), rows)
            target = view(True, flow, stream, LEVEL_SLOT[level] + (d - 1) * rows, rows) if step < 5 else source
            sends.append(remote(flow, stream, source, target, 3 * step - 7 + d, axes[level], sign * d))
        return sends

    def absorb(flow, stream, step):
        for each in copies(flow, stream, step):
            each.wait_recv()
        if step >= 6:
            for each in stores(flow, stream, step - 6):
                each.start()
        if step >= 5:
            return
        if step < 3:
            level, row, brought = 0, chunk(flow, 0, -step - 1), (step,)
        else:
            level = direct_level(step)
            row, brought = chunk(flow, level, 1), (0, 1, 2)
        rows = LEVEL_ROWS[level]
        part = min(rows, PART_ROWS)

        def add(i, carry):
            kept = view(False, flow, stream, pl.multiple_of(row + i * part, 16), part)
            total = kept[ALL].astype(F32)
            for slot in brought:
                total = total + view(True, flow, stream, pl.multiple_of(LEVEL_SLOT[level] + slot * rows + i * part, 16), part)[ALL].astype(F32)
            kept[ALL] = total.astype(BF16)
            return carry

        if rows == part:
            add(0, 0)
        else:
            lax.fori_loop(0, rows // part, add, 0)

    def give(flow, stream, level):
        axes, sign = FLOWS[flow]
        for step in (0, 1, 2) if level == 0 else (level + 2,):
            for each in copies(flow, stream, step):
                each.wait_send()
        for shift in (-sign,) if level == 0 else PEERS:
            tell(free_sem.at[flow, stream, level], neighbour(axes[level], shift))

    def run_op(stream, step):
        ring = stream > 0
        for flow in FLOW_IDS:
            if step > FIRST_STEP[stream]:
                absorb(flow, stream, step - 1)
        for flow in FLOW_IDS:
            if step == 4 and ring:
                give(flow, stream, 0)
            if step == 5:
                give(flow, stream, 1)
                give(flow, stream, 2)
        for flow in FLOW_IDS:
            if step == 5:
                pl.semaphore_wait(free_sem.at[flow, stream, 2], 3)
            if step == 6:
                pl.semaphore_wait(free_sem.at[flow, stream, 1], 3)
            if step == 7 and ring:
                pl.semaphore_wait(free_sem.at[flow, stream, 0], 1)
        if step < STEPS:
            for flow in FLOW_IDS:
                for each in copies(flow, stream, step):
                    each.start()

    def run_point(spot):
        for pair in range(pairs):
            ops = inside.get((pair, spot), [])
            if ops:
                @pl.when(pid == pair)
                def _():
                    for stream, step in ops:
                        run_op(stream, step)

    own_turn = lax.rem(pid, 2) == 1
    spot = pid // 2

    def slot_of(j):
        return 3 * j + 4 * (j // 2)

    def swap_copy(j):
        return pltpu.make_async_remote_copy(
            src_ref=sent.at[j % 2 if isinstance(j, int) else lax.rem(j, 2)], dst_ref=small.at[pl.ds(slot_of(j), 3)],
            send_sem=swap_send.at[j], recv_sem=swap_recv.at[j], device_id=partner, device_id_type=MESH_ID)

    @pl.when(pid == 0)
    def _():
        barrier = pltpu.get_barrier_semaphore()
        for axis in range(3):
            for shift in PEERS:
                tell(barrier, neighbour(axis, shift))
        tell(barrier, partner)
        for each in loads():
            each.start()
        pl.semaphore_wait(barrier, 10)
        for each in loads():
            each.wait()
        da_acc[ALL] = jnp.zeros_like(da_acc)

    run_point(0)
    block = qkv_ref[ALL]
    block_t = block.T
    grad = grad_ref[ALL]
    grad_t = grad.T
    prod_t = grad_t.astype(F32) * out_ref[ALL].T.astype(F32)
    start = start_ref[0:1, :]
    pieces = attn_bwd_head(dim, scale, 0, block, block_t, grad, grad_t, prod_t, start, lse_ref[0, 0:1, :])
    run_point(1)
    pieces += attn_bwd_head(dim, scale, 1, block, block_t, grad, grad_t, prod_t, start, lse_ref[0, 1:2, :])
    dqkv = jnp.concatenate(pieces, axis=1).astype(BF16)
    run_point(2)
    weight = jnp.where(own_turn, wo_ref[ALL], wp_ref[ALL])
    da_acc[ALL] += dot_nt(dqkv, weight)
    run_point(3)

    @pl.when(jnp.logical_not(own_turn))
    def _():
        @pl.when(spot >= 2)
        def _():
            swap_copy(spot - 2).wait_send()

        dw = dot_nn(normed_t_ref[ALL], dqkv).astype(BF16)
        for k in range(3):
            sent[lax.rem(spot, 2), k] = dw[:, k * UNIT : (k + 1) * UNIT]
        swap_copy(spot).start()

    @pl.when(own_turn)
    def _():
        dw = dot_nn(normed_t_ref[ALL], dqkv)
        swap_copy(spot).wait_recv()
        for k in range(3):
            index = slot_of(spot) + k
            small[index] = (dw[:, k * UNIT : (k + 1) * UNIT] + small[index].astype(F32)).astype(BF16)

    @pl.when(pid == pairs - 1)
    def _():
        queue = list(after)

        def advance(count):
            for _ in range(min(count, len(queue))):
                run_op(*queue.pop(0))

        advance(1)
        gain = gain_ref[0:1, :]

        def norm_tile(i, total):
            at = pl.ds(pl.multiple_of(i * UNIT, UNIT), UNIT)
            x_tile = x_ref[at, :]
            mean, inv_std = norm_stats(x_tile)
            back, gain_part = norm_backward(da_acc[at, :].astype(BF16), x_tile, mean, inv_std, gain)
            dx_buf[at, :] = (gx_ref[at, :].astype(F32) + back).astype(BF16)
            return total + gain_part

        gain_one = lax.fori_loop(0, x_ref.shape[0] // UNIT, norm_tile, jnp.zeros_like(gain))
        for k in range(8):
            gains[0, core, k : k + 1, :] = gain_one[:, k * UNIT : (k + 1) * UNIT]
            gains[0, core, k + 8 : k + 9, :] = gain_two_ref[0:1, k * UNIT : (k + 1) * UNIT]
        advance(1)
        dx_local = pltpu.make_async_copy(dx_buf, dx_out.at[core], dx_sem.at[0])
        dx_remote = pltpu.make_async_remote_copy(
            src_ref=dx_buf, dst_ref=dx_out.at[core], send_sem=dx_sem.at[1], recv_sem=dx_sem.at[2], device_id=partner, device_id_type=MESH_ID)
        dx_local.start()
        dx_remote.start()

        def gain_copy(stage, slot, where_to, lane):
            return pltpu.make_async_remote_copy(
                src_ref=gains.at[stage, slot], dst_ref=gains.at[stage, slot], send_sem=gain_send.at[stage, lane], recv_sem=gain_recv.at[stage, slot],
                device_id=where_to, device_id_type=MESH_ID)

        for stage in range(4):
            if stage == 0:
                members, spot = 2, core
                others = [(partner, 1 - core)]
            else:
                members, spot = RING, coords[stage - 1]
                others = [(neighbour(stage - 1, d), lax.rem(spot + d, RING)) for d in PEERS]
            for lane, (target, _) in enumerate(others):
                gain_copy(stage, spot, target, lane).start()
            advance(2)
            for lane, (target, slot) in enumerate(others):
                gain_copy(stage, slot, target, lane).wait_recv()
                gain_copy(stage, spot, target, lane).wait_send()
            total = gains[stage, 0]
            for member in range(1, members):
                total = total + gains[stage, member]
            if stage < 3:
                gains[stage + 1, coords[stage]] = total
            else:
                gains_out[ALL] = total
        advance(len(queue))
        swap_copy(half - 2).wait_send()
        swap_copy(half - 1).wait_send()
        dx_local.wait()
        dx_remote.wait()
        for stream in range(STREAMS):
            for flow in FLOW_IDS:
                for step in range(5, STEPS):
                    for each in copies(flow, stream, step):
                        each.wait_send()
                for turn in range(4):
                    for each in stores(flow, stream, turn):
                        each.wait()


def backward_tail(dim, scale, start, qkv, out, grad, lse, w_peer, w_own, normed_t, x_rows, gx_rows, gain_one, gain_two_grad, part, grads_out, big_shapes):
    seq, hidden = x_rows.shape
    width = 6 * dim
    half = w_own.shape[1] // width
    pairs = 2 * half
    any_spec = pl.BlockSpec(memory_space=pl.ANY)
    by_pair = lambda i: (0, order(i))
    order = lambda i: lax.rem(i, 2) * half + i // 2
    row = lambda value: jnp.broadcast_to(value.astype(F32), (8, hidden))
    return pl.pallas_call(
        functools.partial(tail_kernel, dim, scale, pairs),
        grid=(pairs,),
        in_specs=[
            whole((8, seq)),
            pl.BlockSpec((seq, width), by_pair),
            pl.BlockSpec((seq, 2 * dim), by_pair),
            pl.BlockSpec((seq, 2 * dim), by_pair),
            pl.BlockSpec((1, 8, seq), lambda i: (order(i), 0, 0)),
            *[pl.BlockSpec((hidden, width), lambda i: (0, i // 2))] * 2,
            whole((hidden, seq)),
            whole((seq, hidden)),
            whole((seq, hidden)),
            whole((8, hidden)),
            whole((8, hidden)),
        ] + [any_spec] * 2,
        out_specs=[any_spec] * 5 + [pl.BlockSpec((16, UNIT), FIRST)],
        out_shape=[jax.ShapeDtypeStruct(shape, BF16) for shape in (*big_shapes, grads_out.shape)] + [
            jax.ShapeDtypeStruct((hidden, half * width), BF16),
            jax.ShapeDtypeStruct((2, seq, hidden), BF16),
            jax.ShapeDtypeStruct((16, UNIT), F32),
        ],
        scratch_shapes=[
            pltpu.VMEM((N_FLOWS, FLOW_ROWS, BIG_COLS), BF16),
            pltpu.VMEM((N_FLOWS, SLOT_ROWS - BIG_SLOT_BASE, BIG_COLS), BF16),
            pltpu.VMEM((16, FLOW_ROWS, UNIT), BF16),
            pltpu.VMEM((16, SLOT_ROWS, UNIT), BF16),
            pltpu.VMEM((2, 3, FLOW_ROWS, UNIT), BF16),
            pltpu.VMEM((seq, hidden), F32),
            pltpu.VMEM((seq, hidden), BF16),
            pltpu.VMEM((4, RING, 16, UNIT), F32),
            pltpu.SemaphoreType.DMA((N_FLOWS, STREAMS, SEMS)),
            pltpu.SemaphoreType.DMA((N_FLOWS, STREAMS, SEMS)),
            pltpu.SemaphoreType.DMA((14,)),
            pltpu.SemaphoreType.DMA((N_FLOWS, STREAMS, 4, 3)),
            pltpu.SemaphoreType.DMA((half,)),
            pltpu.SemaphoreType.DMA((half,)),
            pltpu.SemaphoreType.DMA((3,)),
            pltpu.SemaphoreType.DMA((4, 3)),
            pltpu.SemaphoreType.DMA((4, RING)),
            pltpu.SemaphoreType.REGULAR((N_FLOWS, STREAMS, 3)),
        ],
        compiler_params=pltpu.CompilerParams(collective_id=0, has_side_effects=True, vmem_limit_bytes=TAIL_VMEM),
        cost_estimate=cost(pairs * seq * seq * hidden),
        name="backward_tail",
    )(start, qkv, out, grad, lse, w_peer, w_own, normed_t, x_rows, gx_rows, row(gain_one[None, :]), row(gain_two_grad), part, grads_out)


def solution(mesh):
    batch_spec = P(("pod", "dp"))
    columns = P(None, "tp")

    def local_step(x_in, seg_ids, gain_one, gain_two, w_qkv, w_out, w_up, w_down, grad_y):
        heads_loc, dim, hidden = w_out.shape
        scale = dim ** -0.5
        swap = lambda value: lax.ppermute(value, "tp", SWAP)
        mine = lax.axis_index("tp")
        own_row = lambda value: lax.dynamic_index_in_dim(value, mine, 0, keepdims=False)

        w_out = w_out.reshape(heads_loc * dim, hidden)
        wqkv_p = swap(w_qkv)
        wout_p = swap(w_out)
        wup_p = swap(w_up)
        wdown_p = swap(w_down)
        x_rows = own_row(x_in)
        grad_rows = own_row(grad_y)
        seg = own_row(seg_ids)
        seq = x_rows.shape[0]
        start = jnp.sum((seg[None, :] < seg[:, None]).astype(jnp.int32), axis=1)
        start = jnp.broadcast_to(start[None, :], (8, seq))

        mean_a, inv_a = norm_stats(x_rows)
        normed_a = norm_apply(x_rows, mean_a, inv_a, gain_one)
        qkv, attn, lse, normed_t = attention_forward(start, normed_a, wqkv_p, w_qkv, dim, scale)
        wout_all = jnp.concatenate([wout_p, w_out], axis=0)
        part_one = dot_nn(attn, wout_all).astype(BF16)
        x_one = (x_rows.astype(F32) + part_one.astype(F32)).astype(BF16)
        mean_b, inv_b = norm_stats(x_one)
        normed_b = norm_apply(x_one, mean_b, inv_b, gain_two)

        ffn_loc = w_up.shape[1]
        act, dpre = mlp_mid(normed_b, grad_rows, wup_p, w_up, wdown_p, w_down)
        sent_down = swap(dot_tn(act[:, :ffn_loc], grad_rows).astype(BF16))
        sent_up = swap(dot_tn(normed_b, dpre[:, :ffn_loc]).astype(BF16))
        grad_down = (dot_tn(act[:, ffn_loc:], grad_rows) + sent_down.astype(F32)).astype(BF16)
        grad_up = (dot_tn(normed_b, dpre[:, ffn_loc:]) + sent_up.astype(F32)).astype(BF16)
        grad_norm_b, part, y_out = mlp_out(act, dpre, wdown_p, w_down, wup_p, w_up, x_one, (grad_up, grad_down))
        back_b, gain_grad_two = norm_backward(grad_norm_b, x_one, mean_b, inv_b, gain_two)
        grad_x_one = (grad_rows.astype(F32) + back_b).astype(BF16)
        grad_wout = dot_tn(attn, grad_x_one)
        rows_loc = heads_loc * dim
        sent_out = swap(grad_wout[:rows_loc].astype(BF16))
        grad_out_w = (grad_wout[rows_loc:] + sent_out.astype(F32)).astype(BF16)
        dattn = dot_nt(grad_x_one, wout_all).astype(BF16)

        sum_up, sum_down, sum_out, sum_qkv, grad_x, gain_sums = backward_tail(
            dim, scale, start, qkv, attn, dattn, lse, wqkv_p, w_qkv, normed_t, x_rows, grad_x_one, gain_one, gain_grad_two, part, grad_out_w, (grad_up.shape, grad_down.shape))
        gain_sums = gain_sums.reshape(2, hidden).astype(BF16)
        return (
            y_out,
            grad_x,
            gain_sums[0],
            gain_sums[1],
            sum_qkv,
            sum_out.reshape(heads_loc, dim, hidden),
            sum_up,
            sum_down,
        )

    return jax.shard_map(
        local_step,
        mesh=mesh,
        in_specs=(batch_spec, batch_spec, P(), P(), columns, P("tp"), columns, P("tp"), batch_spec),
        out_specs=(batch_spec, batch_spec, P("pod"), P("pod"), P("pod", "tp"), P(("pod", "tp")), P("pod", "tp"), P(("pod", "tp"))),
        check_vma=False,
    )
```

```python
import functools
import math

import jax
import jax.numpy as jnp
from jax import lax
from jax.experimental import pallas as pl
from jax.experimental.pallas import tpu as pltpu
from jax.sharding import PartitionSpec as P

EPS_NORM = 1e-5
NEG_LARGE = -1e30
LOG2E = math.log2(math.e)
SWAP = [(0, 1), (1, 0)]
TILE = 256
FWD_TILE = 512
UNIT = 128
BF16 = jnp.bfloat16
F32 = jnp.float32
ALL = ...
ROW = dict(axis=-1, keepdims=True)
COL = dict(axis=0, keepdims=True)


def norm_stats(x_rows):
    x_f32 = x_rows.astype(F32)
    mean = jnp.mean(x_f32, **ROW)
    centered = x_f32 - mean
    inv_std = lax.rsqrt(jnp.mean(centered * centered, **ROW) + EPS_NORM)
    return mean, inv_std


def norm_apply(x_rows, mean, inv_std, gain_vec):
    return ((x_rows.astype(F32) - mean) * inv_std * gain_vec.astype(F32)).astype(BF16)


def norm_backward(grad_out, x_rows, mean, inv_std, gain_vec):
    grad_f32 = grad_out.astype(F32)
    x_hat = (x_rows.astype(F32) - mean) * inv_std
    grad_gain = jnp.sum(grad_f32 * x_hat, **COL)
    grad_hat = grad_f32 * gain_vec.astype(F32)
    mean_one = jnp.mean(grad_hat, **ROW)
    mean_two = jnp.mean(grad_hat * x_hat, **ROW)
    return inv_std * (grad_hat - mean_one - x_hat * mean_two), grad_gain


def cost(flops):
    return pl.CostEstimate(flops=flops, bytes_accessed=flops // UNIT, transcendentals=flops // UNIT)


def dot_nn(lhs, rhs):
    return lax.dot_general(lhs, rhs, (((1,), (0,)), ((), ())), preferred_element_type=F32)


def dot_nt(lhs, rhs):
    return lax.dot_general(lhs, rhs, (((1,), (1,)), ((), ())), preferred_element_type=F32)


def dot_tn(lhs, rhs):
    return lax.dot_general(lhs, rhs, (((0,), (0,)), ((), ())), preferred_element_type=F32)


FIRST = lambda i: (0, 0)
ACROSS = lambda i: (0, i)
VMEM_LIMIT = 56 * 1024 * 1024
TAIL_VMEM = 63 * 1024 * 1024


def head_parts(dim, head, width, take):
    base = head * (width // 2)
    return [take(lo, lo + dim) for lo in range(base, base + width // 2, dim)]


def attn_fwd_kernel(dim, scale, start_ref, normed_ref, wp_ref, wo_ref, qkv_ref, out_ref, lse_ref, normed_t_ref):
    seq = qkv_ref.shape[0]
    step = pl.program_id(0)
    half = pl.num_programs(0) // 2

    @pl.when(step == 0)
    def _():
        normed_t_ref[ALL] = normed_ref[ALL].T

    weight = jnp.where(step < half, wp_ref[ALL], wo_ref[ALL])
    block = dot_nn(normed_ref[ALL], weight).astype(BF16)
    qkv_ref[ALL] = block
    block_t = block.T
    start = start_ref[0:1, :]
    heads_t = []
    for head in range(2):
        _, k_rows, _ = head_parts(dim, head, block.shape[1], lambda lo, hi: block[:, lo:hi])
        q_cols, _, v_cols = head_parts(dim, head, block.shape[1], lambda lo, hi: block_t[lo:hi])
        strips = []
        for i in range(seq // FWD_TILE):
            lo, hi = i * FWD_TILE, (i + 1) * FWD_TILE
            scores = dot_nn(k_rows[:hi], q_cols[:, lo:hi]) * (scale * LOG2E)
            k_pos = lax.broadcasted_iota(jnp.int32, (hi, FWD_TILE), 0)
            allowed = k_pos >= start[:, lo:hi]
            q_pos = lax.broadcasted_iota(jnp.int32, (FWD_TILE, FWD_TILE), 1) + lo
            diag = jnp.where(allowed[lo:] & (k_pos[lo:] <= q_pos), scores[lo:], NEG_LARGE)
            if lo:
                body = jnp.where(allowed[:lo], scores[:lo], NEG_LARGE)
                scores = jnp.concatenate([body, diag], axis=0)
            else:
                scores = diag
            top = jnp.max(scores, **COL)
            probs = jnp.exp2(scores - top)
            total = jnp.sum(probs, **COL)
            probs = (probs * (1.0 / total)).astype(BF16)
            strips.append(dot_nn(v_cols[:, :hi], probs))
            lse_ref[0, head : head + 1, lo:hi] = top + jnp.log2(total)
        heads_t.append(jnp.concatenate(strips, axis=1))
    out_ref[ALL] = jnp.concatenate(heads_t, axis=0).T.astype(BF16)


def attention_forward(start, normed, w_peer, w_own, dim, scale):
    seq, hidden = normed.shape
    width = 6 * dim
    half = w_own.shape[1] // width
    pairs = 2 * half
    return pl.pallas_call(
        functools.partial(attn_fwd_kernel, dim, scale),
        grid=(pairs,),
        in_specs=[
            pl.BlockSpec((8, seq), FIRST),
            pl.BlockSpec((seq, hidden), FIRST),
            *half_specs((hidden, width), half, 1),
        ],
        out_specs=[
            pl.BlockSpec((seq, width), ACROSS),
            pl.BlockSpec((seq, 2 * dim), ACROSS),
            pl.BlockSpec((1, 8, seq), lambda i: (i, 0, 0)),
            pl.BlockSpec((hidden, seq), FIRST),
        ],
        out_shape=[
            jax.ShapeDtypeStruct((seq, pairs * width), BF16),
            jax.ShapeDtypeStruct((seq, pairs * 2 * dim), BF16),
            jax.ShapeDtypeStruct((pairs, 8, seq), F32),
            jax.ShapeDtypeStruct((hidden, seq), BF16),
        ],
        compiler_params=pltpu.CompilerParams(vmem_limit_bytes=VMEM_LIMIT),
        cost_estimate=cost(pairs * seq * seq * hidden),
        name="attn_fwd",
    )(start, normed, w_peer, w_own)


def attn_bwd_head(dim, scale, head, block, block_t, grad, grad_t, prod_t, start, lse):
    seq = block.shape[0]
    q_rows, k_rows, v_rows = head_parts(dim, head, block.shape[1], lambda lo, hi: block[:, lo:hi])
    q_cols, k_cols, _ = head_parts(dim, head, block.shape[1], lambda lo, hi: block_t[lo:hi])
    do_rows = grad[:, head * dim : (head + 1) * dim]
    do_cols = grad_t[head * dim : (head + 1) * dim]
    delta = jnp.sum(prod_t[head * dim : (head + 1) * dim], **COL)
    dq_cols = None
    dk_parts, dv_parts = [], []
    for j in range(seq // TILE):
        lo, hi = j * TILE, (j + 1) * TILE
        width = seq - lo
        scores = dot_nn(k_rows[lo:hi], q_cols[:, lo:]) * (scale * LOG2E)
        grad_probs = dot_nn(v_rows[lo:hi], do_cols[:, lo:])
        k_pos = lax.broadcasted_iota(jnp.int32, (TILE, width), 0) + lo
        allowed = k_pos >= start[:, lo:]
        q_pos = lax.broadcasted_iota(jnp.int32, (TILE, TILE), 1) + lo
        probs = jnp.exp2(scores - lse[:, lo:])
        diag = jnp.where(allowed[:, :TILE] & (k_pos[:, :TILE] <= q_pos), probs[:, :TILE], 0.0)
        if width > TILE:
            body = jnp.where(allowed[:, TILE:], probs[:, TILE:], 0.0)
            probs = jnp.concatenate([diag, body], axis=1)
        else:
            probs = diag
        grad_scores = (probs * (grad_probs - delta[:, lo:]) * scale).astype(BF16)
        dv_parts.append(dot_nn(probs.astype(BF16), do_rows[lo:]))
        dk_parts.append(dot_nn(grad_scores, q_rows[lo:]))
        dq_part = dot_nn(k_cols[:, lo:hi], grad_scores)
        if dq_cols is None:
            dq_cols = dq_part
        else:
            dq_cols = jnp.concatenate([dq_cols[:, :lo], dq_cols[:, lo:] + dq_part], axis=1)
    return [dq_cols.T, jnp.concatenate(dk_parts, axis=0), jnp.concatenate(dv_parts, axis=0)]


GELU_A = math.sqrt(2.0 / math.pi)
GELU_B = 0.044715


def mlp_mid_kernel(rows, b_ref, dy_ref, up_p_ref, up_o_ref, down_p_ref, down_o_ref, act_ref, dpre_ref):
    peer = pl.program_id(0) < pl.num_programs(0) // 2
    w_up = jnp.where(peer, up_p_ref[ALL], up_o_ref[ALL])
    w_down = jnp.where(peer, down_p_ref[ALL], down_o_ref[ALL])
    for r in range(b_ref.shape[0] // rows):
        span = pl.ds(r * rows, rows)
        pre = dot_nn(b_ref[span, :], w_up)
        grad_h = dot_nt(dy_ref[span, :], w_down).astype(BF16).astype(F32)
        square = pre * pre
        tanh = jnp.tanh(pre * (GELU_A + (GELU_A * GELU_B) * square))
        cdf = 0.5 + 0.5 * tanh
        act_ref[span, :] = (pre * cdf).astype(BF16)
        slope = cdf + (0.5 * pre) * (1.0 - tanh * tanh) * (GELU_A + (3.0 * GELU_A * GELU_B) * square)
        dpre_ref[span, :] = (grad_h * slope).astype(BF16)


def whole(shape):
    return pl.BlockSpec(shape, lambda i: (0,) * len(shape), pipeline_mode=pl.Buffered(1))


def half_specs(shape, half, axis):
    at = lambda index: (0, index) if axis else (index, 0)
    return [
        pl.BlockSpec(shape, lambda i: at(jnp.minimum(i, half - 1))),
        pl.BlockSpec(shape, lambda i: at(jnp.maximum(i - half, 0))),
    ]


def mlp_mid(normed, grad_rows, up_p, up_o, down_p, down_o, tile_n=512, rows=1024):
    tokens, hidden = normed.shape
    half = up_o.shape[1] // tile_n
    ffn = 2 * up_o.shape[1]
    return pl.pallas_call(
        functools.partial(mlp_mid_kernel, rows),
        grid=(2 * half,),
        in_specs=[pl.BlockSpec((tokens, hidden), FIRST)] * 2 + half_specs((hidden, tile_n), half, 1) + half_specs((tile_n, hidden), half, 0),
        out_specs=[pl.BlockSpec((tokens, tile_n), ACROSS)] * 2,
        out_shape=[jax.ShapeDtypeStruct((tokens, ffn), BF16)] * 2,
        compiler_params=pltpu.CompilerParams(vmem_limit_bytes=VMEM_LIMIT),
        cost_estimate=cost(tokens * hidden * ffn),
        name="mlp_mid",
    )(normed, grad_rows, up_p, up_o, down_p, down_o)


MESH_ID = pl.DeviceIdType.MESH
RING = 4
FLOW_ROWS = 1024
BIG_COLS = 6 * UNIT
BIG_BOUNDS = (0, 6, 12, 17, 22, 27, 32)
SMALL_BOUNDS = (None, (0, 2, 4, 6, 8, 9, 10), range(10, 17))
OUT_FIRST = 6
STREAMS = 3
LEVEL_ROWS = (256, 64, 16)
LEVEL_SLOT = (0, 768, 960)
SLOT_ROWS = 1008
BIG_SLOT_BASE = 768
AXIS_STRIDE = (1, 4, 16)
FLOWS = tuple((tuple((first + k) % 3 for k in range(3)), sign) for first in range(3) for sign in (1, -1))
FLOW_IDS = range(len(FLOWS))
PEERS = (1, 2, 3)
N_FLOWS = len(FLOWS)
TOP_ROWS, PART_ROWS = 256, 64
HALF_COLS = 512
STEPS = 10
SEMS = 18
POINTS = 4
FIRST_STEP = (3, 0, 0)
PAIR_US = 9.5
HOP_US = 3.2
STREAM_US = (1.4 * 6, 1.4 * 2, 1.4)
GRADS_UP, GRADS_DOWN = range(2)


def big_width(flow):
    return (BIG_BOUNDS[flow + 1] - BIG_BOUNDS[flow]) * UNIT


def big_pieces(flow):
    first, last = BIG_BOUNDS[flow], BIG_BOUNDS[flow + 1]
    pieces = []
    for array, begin, end in ((GRADS_UP, 0, 16), (GRADS_DOWN, 16, 24), (GRADS_DOWN, 24, 32)):
        lo, hi = max(first, begin), min(last, end)
        if lo < hi:
            pieces.append((array, lo - 16 if array == GRADS_DOWN else lo, (lo - first) * UNIT, (hi - lo) * UNIT))
    return pieces


def hbm_block(refs, piece, row, rows):
    array, local, _, width = piece
    ref = refs[array]
    if array == GRADS_UP:
        return ref.at[pl.ds(row, rows), pl.ds(local * UNIT, width)]
    return ref.at[pl.ds((local // 8) * FLOW_ROWS + row, rows), pl.ds((local % 8) * UNIT, width)]


def tell(semaphore, device):
    pl.semaphore_signal(semaphore, inc=1, device_id=device, device_id_type=MESH_ID)


def ring_tools():
    me = lax.axis_index("dp")
    coords = (lax.rem(me, 4), lax.rem(me // 4, 4), me // 16)

    def neighbour(axis, shift):
        moved = lax.rem(coords[axis] + shift + RING, RING)
        return {"dp": me + (moved - coords[axis]) * AXIS_STRIDE[axis]}

    place, bases = [], []
    for axes, sign in FLOWS:
        spots = [coords[a] if sign > 0 else lax.rem(RING - coords[a], RING) for a in axes]
        base = [0]
        for level in range(2):
            base.append(base[-1] + lax.rem(spots[level] + 1, RING) * LEVEL_ROWS[level])
        place.append(spots)
        bases.append(base)

    def chunk(flow, level, shift):
        index = lax.rem(place[flow][level] + shift + RING, RING)
        return pl.multiple_of(bases[flow][level] + index * LEVEL_ROWS[level], LEVEL_ROWS[level])

    return coords, neighbour, chunk


def mlp_out_kernel(steps, act_ref, dpre_ref, down_p_ref, down_o_ref, up_p_ref, up_o_ref, x_ref, up_hbm, down_hbm, db_ref, part_ref, y_out, own, slots, y_acc, b_acc, y_buf, send_sem, recv_sem, load_sem, y_sem):
    pid = pl.program_id(0)
    core = lax.axis_index("tp")
    partner = {"tp": 1 - core}
    coords, neighbour, chunk = ring_tools()
    ins = (up_hbm, down_hbm)
    rows = TOP_ROWS

    def lanes(flow, stream):
        middle = 3 * UNIT
        return pl.ds(0, middle) if stream == 0 else pl.ds(middle, big_width(flow) - middle)

    def loads(flow, turn):
        row = chunk(flow, 0, -turn)
        return [
            pltpu.make_async_copy(hbm_block(ins, piece, row, rows), own.at[flow, pl.ds(row, rows), pl.ds(piece[2], piece[3])], load_sem.at[flow, turn, k])
            for k, piece in enumerate(big_pieces(flow))
        ]

    def copy(flow, stream, turn):
        axes, sign = FLOWS[flow]
        return pltpu.make_async_remote_copy(
            src_ref=own.at[flow, pl.ds(chunk(flow, 0, -turn), rows), lanes(flow, stream)],
            dst_ref=slots.at[flow, pl.ds(turn * rows, rows), lanes(flow, stream)],
            send_sem=send_sem.at[flow, stream, turn], recv_sem=recv_sem.at[flow, stream, turn],
            device_id=neighbour(axes[0], sign), device_id_type=MESH_ID)

    def run_op(stream, step):
        for flow in FLOW_IDS:
            if step == 0:
                if stream == 0:
                    for each in loads(flow, 0):
                        each.wait()
                continue
            copy(flow, stream, step - 1).wait_recv()
            if stream == 0:
                for each in loads(flow, step):
                    each.wait()
            row = chunk(flow, 0, -step)

            def add(i, carry):
                at = (flow, pl.ds(pl.multiple_of(row + i * PART_ROWS, PART_ROWS), PART_ROWS), lanes(flow, stream))
                total = own[at].astype(F32) + slots[flow, pl.ds(pl.multiple_of((step - 1) * rows + i * PART_ROWS, PART_ROWS), PART_ROWS), lanes(flow, stream)].astype(F32)
                if step == 3:
                    part_ref[flow, pl.ds(pl.multiple_of(i * PART_ROWS, PART_ROWS), PART_ROWS), lanes(flow, stream)] = total.astype(BF16)
                else:
                    own[at] = total.astype(BF16)
                return carry

            lax.fori_loop(0, rows // PART_ROWS, add, 0)
        if step < 3:
            for flow in FLOW_IDS:
                copy(flow, stream, step).start()

    @pl.when(pid == 0)
    def _():
        barrier = pltpu.get_barrier_semaphore()
        for axis in range(3):
            for shift in (1, 3):
                tell(barrier, neighbour(axis, shift))
        tell(barrier, partner)
        for turn in range(4):
            for flow in FLOW_IDS:
                for each in loads(flow, turn):
                    each.start()
        pl.semaphore_wait(barrier, 7)
        y_acc[ALL] = jnp.zeros_like(y_acc)
        b_acc[ALL] = jnp.zeros_like(b_acc)
        run_op(0, 0)
        run_op(1, 0)

    def run_ops(stream):
        for turn in PEERS:
            @pl.when(pid == turn)
            def _():
                run_op(stream, turn)

    run_ops(0)
    peer = pid < steps // 2
    y_acc[ALL] += dot_nn(act_ref[ALL], jnp.where(peer, down_p_ref[ALL], down_o_ref[ALL]))
    run_ops(1)
    y_local = pltpu.make_async_copy(y_buf, y_out.at[core], y_sem.at[0])
    y_remote = pltpu.make_async_remote_copy(
        src_ref=y_buf, dst_ref=y_out.at[core], send_sem=y_sem.at[1], recv_sem=y_sem.at[2], device_id=partner, device_id_type=MESH_ID)

    @pl.when(pid == steps - 1)
    def _():
        def tile(i, carry):
            at = pl.ds(pl.multiple_of(i * UNIT, UNIT), UNIT)
            y_buf[at, :] = (x_ref[at, :].astype(F32) + y_acc[at, :].astype(BF16).astype(F32)).astype(BF16)
            return carry

        lax.fori_loop(0, x_ref.shape[0] // UNIT, tile, 0)
        y_local.start()
        y_remote.start()

    b_acc[ALL] += dot_nt(dpre_ref[ALL], jnp.where(peer, up_p_ref[ALL], up_o_ref[ALL]))

    @pl.when(pid == steps - 1)
    def _():
        db_ref[ALL] = b_acc[ALL].astype(BF16)
        y_local.wait()
        y_remote.wait()
        for flow in FLOW_IDS:
            for stream in range(2):
                for turn in range(3):
                    copy(flow, stream, turn).wait_send()


def mlp_out(act, dpre, down_p, down_o, up_p, up_o, x_one, grads, tile_n=1024):
    tokens, ffn = act.shape
    hidden = x_one.shape[1]
    steps = ffn // tile_n
    any_spec = pl.BlockSpec(memory_space=pl.ANY)
    return pl.pallas_call(
        functools.partial(mlp_out_kernel, steps),
        grid=(steps,),
        in_specs=[pl.BlockSpec((tokens, tile_n), ACROSS)] * 2
        + half_specs((tile_n, hidden), steps // 2, 0) + half_specs((hidden, tile_n), steps // 2, 1) + [whole((tokens, hidden)), any_spec, any_spec],
        out_specs=[whole((tokens, hidden)), whole((N_FLOWS, TOP_ROWS, BIG_COLS)), any_spec],
        out_shape=[
            jax.ShapeDtypeStruct((tokens, hidden), BF16),
            jax.ShapeDtypeStruct((N_FLOWS, TOP_ROWS, BIG_COLS), BF16),
            jax.ShapeDtypeStruct((2, tokens, hidden), BF16),
        ],
        scratch_shapes=[
            pltpu.VMEM((N_FLOWS, FLOW_ROWS, BIG_COLS), BF16),
            pltpu.VMEM((N_FLOWS, 3 * TOP_ROWS, BIG_COLS), BF16),
            pltpu.VMEM((tokens, hidden), F32),
            pltpu.VMEM((tokens, hidden), F32),
            pltpu.VMEM((tokens, hidden), BF16),
            pltpu.SemaphoreType.DMA((N_FLOWS, 2, 3)),
            pltpu.SemaphoreType.DMA((N_FLOWS, 2, 3)),
            pltpu.SemaphoreType.DMA((N_FLOWS, 4, 2)),
            pltpu.SemaphoreType.DMA((3,)),
        ],
        compiler_params=pltpu.CompilerParams(collective_id=1, has_side_effects=True, vmem_limit_bytes=TAIL_VMEM),
        cost_estimate=cost(tokens * hidden * ffn),
        name="mlp_out",
    )(act, dpre, down_p, down_o, up_p, up_o, x_one, *grads)


def plan_ops(pairs):
    inside, after = {}, []
    for stream in range(STREAMS):
        clock = (0.0, pairs // 2 * PAIR_US, pairs * PAIR_US)[stream]
        for step in range(FIRST_STEP[stream], STEPS + 1):
            point = None
            for pair in range(pairs):
                for spot in range(POINTS):
                    at = (pair + (0.0, 0.3, 0.55, 0.8)[spot]) * PAIR_US
                    if point is None and at >= clock - 0.01:
                        point, when = (pair, spot), at
            if point is None:
                when = max(clock, pairs * PAIR_US)
                after.append((when, stream, step))
            else:
                inside.setdefault(point, []).append((stream, step))
            if step < STEPS:
                clock = when + HOP_US + STREAM_US[stream]
    after.sort()
    return inside, [(stream, step) for _, stream, step in after]


def tail_kernel(dim, scale, pairs, *refs):
    (start_ref, qkv_ref, out_ref, grad_ref, lse_ref, wp_ref, wo_ref, normed_t_ref, x_ref, gx_ref, gain_ref, gain_two_ref) = refs[:12]
    (part_ref, out_hbm), outs = refs[12:14], refs[14:16]
    out_sum, qkv_sum, dx_out, gains_out = refs[16:20]
    (own, slots, small, small_slots, sent, da_acc, dx_buf, gains, send_sem, recv_sem, load_sem, store_sem, swap_send, swap_recv, dx_sem, gain_send, gain_recv, free_sem) = refs[20:]
    pid = pl.program_id(0)
    half = pairs // 2
    core = lax.axis_index("tp")
    coords, neighbour, chunk = ring_tools()
    inside, after = plan_ops(pairs)
    partner = {"tp": 1 - core}

    def view(of_slots, flow, stream, row, rows):
        if stream == 0:
            if of_slots:
                return slots.at[flow, pl.ds(row - BIG_SLOT_BASE, rows), pl.ds(0, big_width(flow))]
            return own.at[flow, pl.ds(row, rows), pl.ds(0, big_width(flow))]
        first, last = SMALL_BOUNDS[stream][flow : flow + 2]
        units = pl.ds(first, last - first)
        return (small_slots if of_slots else small).at[units, pl.ds(row, rows), :]

    def loads():
        copies = []
        for flow in FLOW_IDS:
            target = own.at[flow, pl.ds(chunk(flow, 0, 1), TOP_ROWS), :]
            copies.append(pltpu.make_async_copy(part_ref.at[flow], target, load_sem.at[flow]))
        for k in range(4):
            for side in range(2):
                source = out_hbm.at[:, pl.ds((4 * side + k) * UNIT, UNIT)]
                target = small.at[OUT_FIRST + k, pl.ds(side * 512, 512), :]
                copies.append(pltpu.make_async_copy(source, target, load_sem.at[6 + 2 * k + side]))
        return copies

    def stores(flow, stream, turn):
        row = chunk(flow, 0, 1 - turn)
        rows = TOP_ROWS
        copies = []
        if stream > 0:
            for k, index in enumerate(range(*SMALL_BOUNDS[stream][flow : flow + 2])):
                if OUT_FIRST <= index < OUT_FIRST + 4:
                    side = row // 512
                    lane = pl.multiple_of(side * 512 + (index - OUT_FIRST) * UNIT, UNIT)
                    target = out_sum.at[pl.ds(pl.multiple_of(row - side * 512, rows), rows), pl.ds(lane, UNIT)]
                else:
                    unit = index if index < OUT_FIRST else index - 4
                    target = qkv_sum.at[pl.ds(row, rows), pl.ds(unit * UNIT, UNIT)]
                copies.append(pltpu.make_async_copy(small.at[index, pl.ds(row, rows), :], target, store_sem.at[flow, stream, turn, k]))
            return copies
        for k, piece in enumerate(big_pieces(flow)):
            source = own.at[flow, pl.ds(row, rows), pl.ds(piece[2], piece[3])]
            copies.append(pltpu.make_async_copy(source, hbm_block(outs, piece, row, rows), store_sem.at[flow, stream, turn, k]))
        return copies

    def remote(flow, stream, source, target, index, axis, shift):
        return pltpu.make_async_remote_copy(
            src_ref=source, dst_ref=target, send_sem=send_sem.at[flow, stream, index], recv_sem=recv_sem.at[flow, stream, index],
            device_id=neighbour(axis, shift), device_id_type=MESH_ID)

    def direct_level(step):
        return step - 2 if step < 5 else 7 - step

    def copies(flow, stream, step):
        axes, sign = FLOWS[flow]
        if step < 3:
            rows = TOP_ROWS
            source = view(False, flow, stream, chunk(flow, 0, -step), rows)
            return [remote(flow, stream, source, view(True, flow, stream, step * rows, rows), step, axes[0], sign)]
        if step >= 7:
            source = view(False, flow, stream, chunk(flow, 0, 8 - step), TOP_ROWS)
            return [remote(flow, stream, source, source, step + 8, axes[0], sign)]
        level = direct_level(step)
        rows = LEVEL_ROWS[level]
        sends = []
        for d in PEERS:
            source = view(False, flow, stream, chunk(flow, level, d + 1 if step < 5 else 1), rows)
            target = view(True, flow, stream, LEVEL_SLOT[level] + (d - 1) * rows, rows) if step < 5 else source
            sends.append(remote(flow, stream, source, target, 3 * step - 7 + d, axes[level], sign * d))
        return sends

    def absorb(flow, stream, step):
        for each in copies(flow, stream, step):
            each.wait_recv()
        if step >= 6:
            for each in stores(flow, stream, step - 6):
                each.start()
        if step >= 5:
            return
        if step < 3:
            level, row, brought = 0, chunk(flow, 0, -step - 1), (step,)
        else:
            level = direct_level(step)
            row, brought = chunk(flow, level, 1), (0, 1, 2)
        rows = LEVEL_ROWS[level]
        part = min(rows, PART_ROWS)

        def add(i, carry):
            kept = view(False, flow, stream, pl.multiple_of(row + i * part, 16), part)
            total = kept[ALL].astype(F32)
            for slot in brought:
                total = total + view(True, flow, stream, pl.multiple_of(LEVEL_SLOT[level] + slot * rows + i * part, 16), part)[ALL].astype(F32)
            kept[ALL] = total.astype(BF16)
            return carry

        if rows == part:
            add(0, 0)
        else:
            lax.fori_loop(0, rows // part, add, 0)

    def give(flow, stream, level):
        axes, sign = FLOWS[flow]
        for step in (0, 1, 2) if level == 0 else (level + 2,):
            for each in copies(flow, stream, step):
                each.wait_send()
        for shift in (-sign,) if level == 0 else PEERS:
            tell(free_sem.at[flow, stream, level], neighbour(axes[level], shift))

    def run_op(stream, step):
        ring = stream > 0
        for flow in FLOW_IDS:
            if step > FIRST_STEP[stream]:
                absorb(flow, stream, step - 1)
        for flow in FLOW_IDS:
            if step == 4 and ring:
                give(flow, stream, 0)
            if step == 5:
                give(flow, stream, 1)
                give(flow, stream, 2)
        for flow in FLOW_IDS:
            if step == 5:
                pl.semaphore_wait(free_sem.at[flow, stream, 2], 3)
            if step == 6:
                pl.semaphore_wait(free_sem.at[flow, stream, 1], 3)
            if step == 7 and ring:
                pl.semaphore_wait(free_sem.at[flow, stream, 0], 1)
        if step < STEPS:
            for flow in FLOW_IDS:
                for each in copies(flow, stream, step):
                    each.start()

    def run_point(spot):
        for pair in range(pairs):
            ops = inside.get((pair, spot), [])
            if ops:
                @pl.when(pid == pair)
                def _():
                    for stream, step in ops:
                        run_op(stream, step)

    own_turn = lax.rem(pid, 2) == 1
    spot = pid // 2

    def slot_of(j):
        return 3 * j + 4 * (j // 2)

    def swap_copy(j):
        return pltpu.make_async_remote_copy(
            src_ref=sent.at[j % 2 if isinstance(j, int) else lax.rem(j, 2)], dst_ref=small.at[pl.ds(slot_of(j), 3)],
            send_sem=swap_send.at[j], recv_sem=swap_recv.at[j], device_id=partner, device_id_type=MESH_ID)

    @pl.when(pid == 0)
    def _():
        barrier = pltpu.get_barrier_semaphore()
        for axis in range(3):
            for shift in PEERS:
                tell(barrier, neighbour(axis, shift))
        tell(barrier, partner)
        for each in loads():
            each.start()
        pl.semaphore_wait(barrier, 10)
        for each in loads():
            each.wait()
        da_acc[ALL] = jnp.zeros_like(da_acc)

    run_point(0)
    block = qkv_ref[ALL]
    block_t = block.T
    grad = grad_ref[ALL]
    grad_t = grad.T
    prod_t = grad_t.astype(F32) * out_ref[ALL].T.astype(F32)
    start = start_ref[0:1, :]
    pieces = attn_bwd_head(dim, scale, 0, block, block_t, grad, grad_t, prod_t, start, lse_ref[0, 0:1, :])
    run_point(1)
    pieces += attn_bwd_head(dim, scale, 1, block, block_t, grad, grad_t, prod_t, start, lse_ref[0, 1:2, :])
    dqkv = jnp.concatenate(pieces, axis=1).astype(BF16)
    run_point(2)
    weight = jnp.where(own_turn, wo_ref[ALL], wp_ref[ALL])
    da_acc[ALL] += dot_nt(dqkv, weight)
    run_point(3)

    @pl.when(jnp.logical_not(own_turn))
    def _():
        @pl.when(spot >= 2)
        def _():
            swap_copy(spot - 2).wait_send()

        dw = dot_nn(normed_t_ref[ALL], dqkv).astype(BF16)
        for k in range(3):
            sent[lax.rem(spot, 2), k] = dw[:, k * UNIT : (k + 1) * UNIT]
        swap_copy(spot).start()

    @pl.when(own_turn)
    def _():
        dw = dot_nn(normed_t_ref[ALL], dqkv)
        swap_copy(spot).wait_recv()
        for k in range(3):
            index = slot_of(spot) + k
            small[index] = (dw[:, k * UNIT : (k + 1) * UNIT] + small[index].astype(F32)).astype(BF16)

    @pl.when(pid == pairs - 1)
    def _():
        queue = list(after)

        def advance(count):
            for _ in range(min(count, len(queue))):
                run_op(*queue.pop(0))

        advance(1)
        gain = gain_ref[0:1, :]

        def norm_tile(i, total):
            at = pl.ds(pl.multiple_of(i * UNIT, UNIT), UNIT)
            x_tile = x_ref[at, :]
            mean, inv_std = norm_stats(x_tile)
            back, gain_part = norm_backward(da_acc[at, :].astype(BF16), x_tile, mean, inv_std, gain)
            dx_buf[at, :] = (gx_ref[at, :].astype(F32) + back).astype(BF16)
            return total + gain_part

        gain_one = lax.fori_loop(0, x_ref.shape[0] // UNIT, norm_tile, jnp.zeros_like(gain))
        for k in range(8):
            gains[0, core, k : k + 1, :] = gain_one[:, k * UNIT : (k + 1) * UNIT]
            gains[0, core, k + 8 : k + 9, :] = gain_two_ref[0:1, k * UNIT : (k + 1) * UNIT]
        advance(1)
        dx_local = pltpu.make_async_copy(dx_buf, dx_out.at[core], dx_sem.at[0])
        dx_remote = pltpu.make_async_remote_copy(
            src_ref=dx_buf, dst_ref=dx_out.at[core], send_sem=dx_sem.at[1], recv_sem=dx_sem.at[2], device_id=partner, device_id_type=MESH_ID)
        dx_local.start()
        dx_remote.start()

        def gain_copy(stage, slot, where_to, lane):
            return pltpu.make_async_remote_copy(
                src_ref=gains.at[stage, slot], dst_ref=gains.at[stage, slot], send_sem=gain_send.at[stage, lane], recv_sem=gain_recv.at[stage, slot],
                device_id=where_to, device_id_type=MESH_ID)

        for stage in range(4):
            if stage == 0:
                members, spot = 2, core
                others = [(partner, 1 - core)]
            else:
                members, spot = RING, coords[stage - 1]
                others = [(neighbour(stage - 1, d), lax.rem(spot + d, RING)) for d in PEERS]
            for lane, (target, _) in enumerate(others):
                gain_copy(stage, spot, target, lane).start()
            advance(2)
            for lane, (target, slot) in enumerate(others):
                gain_copy(stage, slot, target, lane).wait_recv()
                gain_copy(stage, spot, target, lane).wait_send()
            total = gains[stage, 0]
            for member in range(1, members):
                total = total + gains[stage, member]
            if stage < 3:
                gains[stage + 1, coords[stage]] = total
            else:
                gains_out[ALL] = total
        advance(len(queue))
        swap_copy(half - 2).wait_send()
        swap_copy(half - 1).wait_send()
        dx_local.wait()
        dx_remote.wait()
        for stream in range(STREAMS):
            for flow in FLOW_IDS:
                for step in range(5, STEPS):
                    for each in copies(flow, stream, step):
                        each.wait_send()
                for turn in range(4):
                    for each in stores(flow, stream, turn):
                        each.wait()


def backward_tail(dim, scale, start, qkv, out, grad, lse, w_peer, w_own, normed_t, x_rows, gx_rows, gain_one, gain_two_grad, part, grads_out, big_shapes):
    seq, hidden = x_rows.shape
    width = 6 * dim
    half = w_own.shape[1] // width
    pairs = 2 * half
    any_spec = pl.BlockSpec(memory_space=pl.ANY)
    by_pair = lambda i: (0, order(i))
    order = lambda i: lax.rem(i, 2) * half + i // 2
    row = lambda value: jnp.broadcast_to(value.astype(F32), (8, hidden))
    return pl.pallas_call(
        functools.partial(tail_kernel, dim, scale, pairs),
        grid=(pairs,),
        in_specs=[
            whole((8, seq)),
            pl.BlockSpec((seq, width), by_pair),
            pl.BlockSpec((seq, 2 * dim), by_pair),
            pl.BlockSpec((seq, 2 * dim), by_pair),
            pl.BlockSpec((1, 8, seq), lambda i: (order(i), 0, 0)),
            *[pl.BlockSpec((hidden, width), lambda i: (0, i // 2))] * 2,
            whole((hidden, seq)),
            whole((seq, hidden)),
            whole((seq, hidden)),
            whole((8, hidden)),
            whole((8, hidden)),
        ] + [any_spec] * 2,
        out_specs=[any_spec] * 5 + [pl.BlockSpec((16, UNIT), FIRST)],
        out_shape=[jax.ShapeDtypeStruct(shape, BF16) for shape in (*big_shapes, grads_out.shape)] + [
            jax.ShapeDtypeStruct((hidden, half * width), BF16),
            jax.ShapeDtypeStruct((2, seq, hidden), BF16),
            jax.ShapeDtypeStruct((16, UNIT), F32),
        ],
        scratch_shapes=[
            pltpu.VMEM((N_FLOWS, FLOW_ROWS, BIG_COLS), BF16),
            pltpu.VMEM((N_FLOWS, SLOT_ROWS - BIG_SLOT_BASE, BIG_COLS), BF16),
            pltpu.VMEM((16, FLOW_ROWS, UNIT), BF16),
            pltpu.VMEM((16, SLOT_ROWS, UNIT), BF16),
            pltpu.VMEM((2, 3, FLOW_ROWS, UNIT), BF16),
            pltpu.VMEM((seq, hidden), F32),
            pltpu.VMEM((seq, hidden), BF16),
            pltpu.VMEM((4, RING, 16, UNIT), F32),
            pltpu.SemaphoreType.DMA((N_FLOWS, STREAMS, SEMS)),
            pltpu.SemaphoreType.DMA((N_FLOWS, STREAMS, SEMS)),
            pltpu.SemaphoreType.DMA((14,)),
            pltpu.SemaphoreType.DMA((N_FLOWS, STREAMS, 4, 3)),
            pltpu.SemaphoreType.DMA((half,)),
            pltpu.SemaphoreType.DMA((half,)),
            pltpu.SemaphoreType.DMA((3,)),
            pltpu.SemaphoreType.DMA((4, 3)),
            pltpu.SemaphoreType.DMA((4, RING)),
            pltpu.SemaphoreType.REGULAR((N_FLOWS, STREAMS, 3)),
        ],
        compiler_params=pltpu.CompilerParams(collective_id=0, has_side_effects=True, vmem_limit_bytes=TAIL_VMEM),
        cost_estimate=cost(pairs * seq * seq * hidden),
        name="backward_tail",
    )(start, qkv, out, grad, lse, w_peer, w_own, normed_t, x_rows, gx_rows, row(gain_one[None, :]), row(gain_two_grad), part, grads_out)


def solution(mesh):
    batch_spec = P(("pod", "dp"))
    columns = P(None, "tp")

    def local_step(x_in, seg_ids, gain_one, gain_two, w_qkv, w_out, w_up, w_down, grad_y):
        heads_loc, dim, hidden = w_out.shape
        scale = dim ** -0.5
        swap = lambda value: lax.ppermute(value, "tp", SWAP)
        mine = lax.axis_index("tp")
        own_row = lambda value: lax.dynamic_index_in_dim(value, mine, 0, keepdims=False)

        w_out = w_out.reshape(heads_loc * dim, hidden)
        wqkv_p = swap(w_qkv)
        wout_p = swap(w_out)
        wup_p = swap(w_up)
        wdown_p = swap(w_down)
        x_rows = own_row(x_in)
        grad_rows = own_row(grad_y)
        seg = own_row(seg_ids)
        seq = x_rows.shape[0]
        start = jnp.sum((seg[None, :] < seg[:, None]).astype(jnp.int32), axis=1)
        start = jnp.broadcast_to(start[None, :], (8, seq))

        mean_a, inv_a = norm_stats(x_rows)
        normed_a = norm_apply(x_rows, mean_a, inv_a, gain_one)
        qkv, attn, lse, normed_t = attention_forward(start, normed_a, wqkv_p, w_qkv, dim, scale)
        wout_all = jnp.concatenate([wout_p, w_out], axis=0)
        part_one = dot_nn(attn, wout_all).astype(BF16)
        x_one = (x_rows.astype(F32) + part_one.astype(F32)).astype(BF16)
        mean_b, inv_b = norm_stats(x_one)
        normed_b = norm_apply(x_one, mean_b, inv_b, gain_two)

        ffn_loc = w_up.shape[1]
        act, dpre = mlp_mid(normed_b, grad_rows, wup_p, w_up, wdown_p, w_down)
        sent_down = swap(dot_tn(act[:, :ffn_loc], grad_rows).astype(BF16))
        sent_up = swap(dot_tn(normed_b, dpre[:, :ffn_loc]).astype(BF16))
        grad_down = (dot_tn(act[:, ffn_loc:], grad_rows) + sent_down.astype(F32)).astype(BF16)
        grad_up = (dot_tn(normed_b, dpre[:, ffn_loc:]) + sent_up.astype(F32)).astype(BF16)
        grad_norm_b, part, y_out = mlp_out(act, dpre, wdown_p, w_down, wup_p, w_up, x_one, (grad_up, grad_down))
        back_b, gain_grad_two = norm_backward(grad_norm_b, x_one, mean_b, inv_b, gain_two)
        grad_x_one = (grad_rows.astype(F32) + back_b).astype(BF16)
        grad_wout = dot_tn(attn, grad_x_one)
        rows_loc = heads_loc * dim
        sent_out = swap(grad_wout[:rows_loc].astype(BF16))
        grad_out_w = (grad_wout[rows_loc:] + sent_out.astype(F32)).astype(BF16)
        dattn = dot_nt(grad_x_one, wout_all).astype(BF16)

        sum_up, sum_down, sum_out, sum_qkv, grad_x, gain_sums = backward_tail(
            dim, scale, start, qkv, attn, dattn, lse, wqkv_p, w_qkv, normed_t, x_rows, grad_x_one, gain_one, gain_grad_two, part, grad_out_w, (grad_up.shape, grad_down.shape))
        gain_sums = gain_sums.reshape(2, hidden).astype(BF16)
        return (
            y_out,
            grad_x,
            gain_sums[0],
            gain_sums[1],
            sum_qkv,
            sum_out.reshape(heads_loc, dim, hidden),
            sum_up,
            sum_down,
        )

    return jax.shard_map(
        local_step,
        mesh=mesh,
        in_specs=(batch_spec, batch_spec, P(), P(), columns, P("tp"), columns, P("tp"), batch_spec),
        out_specs=(batch_spec, batch_spec, P("pod"), P("pod"), P("pod", "tp"), P(("pod", "tp")), P("pod", "tp"), P(("pod", "tp"))),
        check_vma=False,
    )
```
